32 devices in a mesh: tm: 2 (over core), space: 16 (over z, y, x).
Axes of the slice: x: 2, y: 2, z: 4, core: 2. Of those that a mesh axis runs over, the one named last changes fastest.
Arguments:
- fine: bfloat16 [8, 64, 256, 256], P('tm', 'space'), may hold values from -6 to 6
- coarse: bfloat16 [8, 32, 128, 256], P('tm', 'space'), may hold values from -6 to 6
- w_query: bfloat16 [256, 256], replicated, may hold values from -24 to 24
- w_key: bfloat16 [256, 256], replicated, may hold values from -0.375 to 0.375
- w_value: bfloat16 [256, 256], replicated, may hold values from -0.375 to 0.375
- w_out: bfloat16 [256, 256], replicated, may hold values from -0.375 to 0.375
- conv_first: bfloat16 [3, 3, 256, 256], replicated, may hold values from -0.125 to 0.125
- conv_second: bfloat16 [3, 3, 256, 256], replicated, may hold values from -0.125 to 0.125
Outputs:
- joined: bfloat16 [8, 64, 256, 256], P('tm', 'space')
The draws below stay inside these ranges and needn't reach their ends.
All inputs are finite; a program needn't handle non-finite values.
Results may differ from the reference program's by a relative error of at most 0.009.
Values may be sent and summed in bfloat16 or wider, within the bound.
A program may use at most 128 MiB of HBM per device.

```python
import jax
import jax.numpy as jnp
from jax import lax

C = 256
HEADS = 8
W = 256
FRAMES = 8
H = 64


def draw_w_query(key, part):
    base = jax.random.normal(jax.random.fold_in(key, 11), (C, C), jnp.float32) / jnp.sqrt(jnp.float32(C))
    base = jnp.clip(base, -6.0 / jnp.sqrt(jnp.float32(C)), 6.0 / jnp.sqrt(jnp.float32(C)))
    logs = jax.random.uniform(jax.random.fold_in(key, 12), (HEADS,), jnp.float32, jnp.log(0.5), jnp.log(3.0))
    columns = jnp.repeat(jnp.exp(logs), C // HEADS)
    return (base * columns[None, :]).astype(jnp.bfloat16)


def shard_levels(own_key, extent, split, least, high):
    loudness, own = 1.0, jax.random.fold_in(own_key, 6)
    for axis_at, blocks in split:
        heights = jnp.exp(jax.random.uniform(jax.random.fold_in(own, axis_at), (blocks,), jnp.float32, least / len(split), high / len(split)))
        loudness = loudness * jnp.repeat(heights, extent[axis_at] // blocks).reshape([-1 if axis == axis_at else 1 for axis in range(len(extent))])
    return loudness


def scatter_about(own_key, extent, deviation, reach, shards=(), kind=jnp.bfloat16):
    entries = jax.random.normal(own_key, extent, jnp.float32) * deviation
    if len(shards) > 0:
        entries = shard_levels(own_key, extent, shards, -0.22, 0.18) * entries
    return jnp.clip(entries, min=-reach, max=reach).astype(kind)


def setup_inputs(seed: int = 0) -> dict:
    arg_keys = jax.random.split(jax.random.key(seed), 9)
    return {
        "fine": scatter_about(arg_keys[0], (FRAMES, H, W, C), 1.0, 6.0, ((0, 2), (1, 16))),
        "coarse": scatter_about(arg_keys[1], (FRAMES, H // 2, W // 2, C), 1.0, 6.0, ((0, 2), (1, 16))),
        "w_query": draw_w_query(jax.random.fold_in(arg_keys[8], 71), 0),
        "w_key": scatter_about(arg_keys[3], (C, C), C ** -0.5, 0.375),
        "w_value": scatter_about(arg_keys[4], (C, C), C ** -0.5, 0.375),
        "w_out": scatter_about(arg_keys[5], (C, C), C ** -0.5, 0.375),
        "conv_first": scatter_about(arg_keys[6], (3, 3, C, C), (9 * C) ** -0.5, 0.125),
        "conv_second": scatter_about(arg_keys[7], (3, 3, C, C), (9 * C) ** -0.5, 0.125),
    }


def encode(frame_ids, width):
    half = width // 2
    index = jnp.arange(half, dtype=jnp.float32)
    inverse = jnp.exp(-jnp.log(10000.0) * 2.0 * index / width)
    angles = frame_ids.astype(jnp.float32)[:, None] * inverse[None, :]
    return jnp.concatenate([jnp.sin(angles), jnp.cos(angles)], axis=1)

def normalize(features, frame_ids):
    width = features.shape[-1]
    hidden = features.astype(jnp.float32) + encode(frame_ids, width)[:, None, None, :]
    center = hidden - lax.optimization_barrier(jnp.mean(hidden, axis=-1, keepdims=True))
    spread = lax.optimization_barrier(jnp.mean(center * center, axis=-1, keepdims=True))
    return (center * lax.rsqrt(spread + 1e-05)).astype(jnp.bfloat16)

def project(normed, weight):
    shape = normed.shape
    flat = normed.reshape(-1, shape[-1])
    return jnp.dot(flat, weight, preferred_element_type=jnp.float32).astype(jnp.bfloat16).reshape(shape)

def attend(query, key, value):
    frames, rows, cols, width = query.shape
    depth = width // HEADS
    query_heads = query.reshape(frames, rows * cols, HEADS, depth).astype(jnp.float32)
    key_heads = key.reshape(key.shape[0], rows * cols, HEADS, depth).astype(jnp.float32)
    value_heads = value.reshape(value.shape[0], rows * cols, HEADS, depth).astype(jnp.float32)
    scores = jnp.einsum('qphd,kphd->qkhp', query_heads, key_heads) / jnp.sqrt(jnp.float32(depth))
    weights = jax.nn.softmax(scores, axis=1).astype(jnp.bfloat16)
    attended = jnp.einsum('qkhp,kphd->qphd', weights.astype(jnp.float32), value_heads)
    return attended.astype(jnp.bfloat16).reshape(frames, rows, cols, width)

def convolve(features, weight):
    return lax.conv_general_dilated(features.astype(jnp.float32), weight.astype(jnp.float32), (1, 1), 'SAME', dimension_numbers=('NHWC', 'HWIO', 'NHWC'), precision=lax.Precision.HIGHEST)

def double(extended, axis):
    count = extended.shape[axis] - 2
    middle = lax.slice_in_dim(extended, 1, count + 1, axis=axis)
    before = lax.slice_in_dim(extended, 0, count, axis=axis)
    after = lax.slice_in_dim(extended, 2, count + 2, axis=axis)
    even = 0.75 * middle + 0.25 * before
    odd = 0.75 * middle + 0.25 * after
    stacked = jnp.stack([even, odd], axis=axis + 1)
    shape = list(middle.shape)
    shape[axis] = 2 * count
    return stacked.reshape(shape)

def upsample(coarse):
    values = coarse.astype(jnp.float32)
    extended = jnp.pad(values, ((0, 0), (1, 1), (0, 0), (0, 0)), mode='edge')
    rows_done = double(extended, 1)
    extended = jnp.pad(rows_done, ((0, 0), (0, 0), (1, 1), (0, 0)), mode='edge')
    return double(extended, 2)

def reference(fine, coarse, w_query, w_key, w_value, w_out, conv_first, conv_second):
    frame_ids = jnp.arange(fine.shape[0], dtype=jnp.int32)
    normed = normalize(fine, frame_ids)
    query = project(normed, w_query)
    key = project(normed, w_key)
    value = project(normed, w_value)
    attended = attend(query, key, value)
    shape = fine.shape
    branch = jnp.dot(attended.reshape(-1, shape[-1]), w_out, preferred_element_type=jnp.float32).reshape(shape)
    moved = (fine.astype(jnp.float32) + branch).astype(jnp.bfloat16)
    first = convolve(jax.nn.relu(moved), conv_first).astype(jnp.bfloat16)
    second = convolve(jax.nn.relu(first), conv_second)
    up = upsample(coarse)
    return (up + moved.astype(jnp.float32) + second).astype(jnp.bfloat16)
```

```python
import functools

import jax
import jax.numpy as jnp
import numpy as np
from jax import lax
from jax.experimental import pallas as pl
from jax.experimental.pallas import tpu as pltpu
from jax.sharding import PartitionSpec as P

HEADS = 8
CHUNKS = 4
STEPS = 8
HALO = 1
LOG2E = 1.4426950408889634
MESH = pl.DeviceIdType.MESH


def encode(frames, width):
    half = width // 2
    inverse = np.exp(-np.log(10000.0) * 2.0 * np.arange(half) / width)
    angles = np.arange(frames)[:, None] * inverse[None, :]
    return np.concatenate([np.sin(angles), np.cos(angles)], axis=1).astype(np.float32)


def lift_matrix(small):
    out = np.arange(2 * small)[:, None]
    source = np.arange(small)[None, :]
    near = out // 2
    far = np.clip(np.where(out % 2 == 0, near - 1, near + 1), 0, small - 1)
    base = 0.75 * (source == near) + 0.25 * (source == far)
    return np.concatenate([0.75 * base, 0.25 * base], axis=1).astype(jnp.bfloat16)


def attention(mine, others, pos, wq_ref, wk_ref, wv_ref, wo_ref):
    own, (tile, width) = len(mine), mine[0].shape
    depth = width // HEADS
    scale = LOG2E / (float(depth) ** 0.5)
    normed = []
    for x, place in zip(mine + others, pos):
        hidden = x.astype(jnp.float32) + place
        center = hidden - jnp.mean(hidden, axis=-1, keepdims=True)
        spread = jnp.mean(center * center, axis=-1, keepdims=True)
        normed.append((center * lax.rsqrt(spread + 1e-05)).astype(jnp.bfloat16))
    flat = jnp.concatenate(normed, axis=0)
    query = jnp.dot(flat[: own * tile], wq_ref[...], preferred_element_type=jnp.float32)
    query = (query * scale).astype(jnp.bfloat16).reshape(own, tile, width)
    key = jnp.dot(flat, wk_ref[...], preferred_element_type=jnp.float32).astype(jnp.bfloat16)
    value = jnp.dot(flat, wv_ref[...], preferred_element_type=jnp.float32).astype(jnp.bfloat16)
    rows = lax.broadcasted_iota(jnp.int32, (width, width), 0) // depth
    cols = lax.broadcasted_iota(jnp.int32, (width, width), 1) // depth
    blocks = jnp.where(rows == cols, 1.0, 0.0).astype(jnp.bfloat16)
    scores = []
    for at in range(len(normed)):
        product = query * key[at * tile : (at + 1) * tile][None]
        scores.append(jnp.dot(product.reshape(own * tile, width), blocks, preferred_element_type=jnp.float32))
    largest = functools.reduce(jnp.maximum, scores)
    total, summed = None, None
    for at, score in enumerate(scores):
        power = jnp.exp2(score - largest).reshape(own, tile, width)
        term = power * value[at * tile : (at + 1) * tile].astype(jnp.float32)[None]
        total = power if total is None else total + power
        summed = term if summed is None else summed + term
    attended = (summed / total).astype(jnp.bfloat16).reshape(own * tile, width)
    branch = jnp.dot(attended, wo_ref[...], preferred_element_type=jnp.float32)
    return branch.reshape(own, tile, width)


def spread_columns(ref, at, row, cols):
    column = lax.broadcasted_iota(jnp.int32, row.shape, 0)
    left = jnp.where(column == 0, 0.0, pltpu.roll(row, 1, 0))
    right = jnp.where(column == cols - 1, 0.0, pltpu.roll(row, cols - 1, 0))
    width = row.shape[1]
    ref[at * cols : (at + 1) * cols, :width] = left.astype(jnp.bfloat16)
    ref[at * cols : (at + 1) * cols, width : 2 * width] = row.astype(jnp.bfloat16)
    ref[at * cols : (at + 1) * cols, 2 * width :] = right.astype(jnp.bfloat16)


def conv_rows(ref, start, first, last, cols, weight_ref):
    pieces = [ref[(start + step) * cols : (start + step + 1) * cols, :] for step in range(first, last)]
    depth = ref.shape[1]
    return jnp.dot(
        jnp.concatenate(pieces, axis=1), weight_ref[first * depth : last * depth, :], preferred_element_type=jnp.float32
    )


def kernel(
    bands, halves, fine_ref, coarse_ref, pos_hbm, wq_hbm, wk_hbm, wv_hbm, wo_hbm, w1_hbm, w2_hbm, lift_hbm, mine,
    other, moved, coarse, x_ref, f_ref, pos_ref, wq_ref, wk_ref, wv_ref, wo_ref, w1_ref, w2_ref, lift_ref,
    edges, part_out, part_in,
    weight_sems, local_sems, fine_send, fine_recv, halo_send, halo_recv, part_send, part_recv,
):
    own, rows, cols, width = mine.shape
    half = rows // 2
    span = cols // CHUNKS
    thin = cols // STEPS
    early = own // 2
    groups = [(0, thin), (thin, 3 * thin), (4 * thin, cols - 4 * thin)]
    slabs = [(row, 1, at, size) for at, size in groups for row in (0, rows - 1)]
    slabs += [(1, rows - 2, chunk * span, span) for chunk in range(CHUNKS)]
    place, core = lax.axis_index("space"), lax.axis_index("tm")
    has_before, has_after = place > 0, place < bands - 1

    def mine_copy(slab):
        row, count, at, size = slabs[slab]
        where = (slice(None), pl.ds(row, count), pl.ds(at, size))
        return pltpu.make_async_copy(fine_ref.at[where], mine.at[where], local_sems.at[slab])

    def fine_copy(shift, slab):
        row, count, at, size = slabs[slab]
        source = mine if count == 1 else fine_ref
        return pltpu.make_async_remote_copy(
            src_ref=source.at[:, pl.ds(row, count), pl.ds(at, size)],
            dst_ref=other.at[pl.ds((shift - 1) * own, own), pl.ds(row, count), pl.ds(at, size)],
            send_sem=fine_send.at[shift - 1, slab],
            recv_sem=fine_recv.at[shift - 1, slab],
            device_id={"tm": lax.rem(core + halves - shift, halves)},
            device_id_type=MESH,
        )

    def to_after(src, dst, send, recv):
        return pltpu.make_async_remote_copy(
            src_ref=src, dst_ref=dst, send_sem=send, recv_sem=recv, device_id={"space": place + 1}, device_id_type=MESH
        )

    def to_before(src, dst, send, recv):
        return pltpu.make_async_remote_copy(
            src_ref=src, dst_ref=dst, send_sem=send, recv_sem=recv, device_id={"space": place - 1}, device_id_type=MESH
        )

    def part_up(frame):
        return to_after(part_out.at[0, frame], part_in.at[0, frame], part_send.at[0, frame], part_recv.at[0, frame])

    def part_down(frame):
        return to_before(part_out.at[1, frame], part_in.at[1, frame], part_send.at[1, frame], part_recv.at[1, frame])

    def halo_up(frames, span_at, piece):
        return to_after(
            moved.at[frames, rows : rows + HALO, span_at], moved.at[frames, 0:HALO, span_at],
            halo_send.at[0, piece], halo_recv.at[0, piece],
        )

    def halo_down(frames, span_at, piece):
        return to_before(
            moved.at[frames, HALO : 2 * HALO, span_at], moved.at[frames, rows + HALO : rows + 2 * HALO, span_at],
            halo_send.at[1, piece], halo_recv.at[1, piece],
        )

    def both(frames, span_at, piece, act_up, act_down):
        pl.when(has_after)(lambda: act_up(halo_up(frames, span_at, piece)))
        pl.when(has_before)(lambda: act_down(halo_down(frames, span_at, piece)))

    def start(copy):
        copy.start()

    def wait_send(copy):
        copy.wait_send()

    def landed(frames, span_at, piece):
        pl.when(has_before)(lambda: halo_up(frames, span_at, piece).wait_recv())
        pl.when(has_after)(lambda: halo_down(frames, span_at, piece).wait_recv())

    barrier = pltpu.get_barrier_semaphore()
    for shift in range(1, halves):
        pl.semaphore_signal(barrier, inc=1, device_id={"tm": lax.rem(core + shift, halves)}, device_id_type=MESH)

    @pl.when(has_before)
    def _():
        pl.semaphore_signal(barrier, inc=1, device_id={"space": place - 1}, device_id_type=MESH)

    @pl.when(has_after)
    def _():
        pl.semaphore_signal(barrier, inc=1, device_id={"space": place + 1}, device_id_type=MESH)

    motion_weights = [
        pltpu.make_async_copy(src, dst, weight_sems.at[at])
        for at, (src, dst) in enumerate(
            [(pos_hbm, pos_ref), (wq_hbm, wq_ref), (wk_hbm, wk_ref), (wv_hbm, wv_ref), (wo_hbm, wo_ref)]
        )
    ]
    later_weights = [
        pltpu.make_async_copy(src, dst, weight_sems.at[5 + at])
        for at, (src, dst) in enumerate(
            [(lift_hbm, lift_ref), (w1_hbm, w1_ref), (w2_hbm, w2_ref), (coarse_ref, coarse)]
        )
    ]
    for slab in range(2):
        mine_copy(slab).start()
    for copy in motion_weights:
        copy.start()
    for slab in range(2, len(slabs)):
        mine_copy(slab).start()
    for copy in later_weights:
        copy.start()

    @pl.when(jnp.logical_not(has_before))
    def _():
        moved[:, 0:HALO] = jnp.zeros((own, HALO, cols, width), jnp.bfloat16)
        part_in[0] = jnp.zeros((own, cols, width), jnp.bfloat16)

    @pl.when(jnp.logical_not(has_after))
    def _():
        moved[:, rows + HALO :] = jnp.zeros((own, HALO, cols, width), jnp.bfloat16)
        part_in[1] = jnp.zeros((own, cols, width), jnp.bfloat16)

    peers = halves - 1 + has_before.astype(jnp.int32) + has_after.astype(jnp.int32)
    pl.semaphore_wait(barrier, peers)

    for slab in range(len(slabs)):
        if slabs[slab][1] == 1:
            mine_copy(slab).wait()
        for shift in range(1, halves):
            fine_copy(shift, slab).start()
    for copy in motion_weights:
        copy.wait()

    pos = []
    for shift in range(halves):
        for frame in range(own):
            pos.append(pos_ref[pl.ds(lax.rem(core + shift, halves) * own + frame, 1), :])

    def motion_tile(places):
        here = [jnp.concatenate([mine[frame, row, at, :] for row, at in places]) for frame in range(own)]
        there = [
            jnp.concatenate([other[frame, row, at, :] for row, at in places]) for frame in range(own * (halves - 1))
        ]
        branch = attention(here, there, pos, wq_ref, wk_ref, wv_ref, wo_ref)
        for frame in range(own):
            result = (here[frame].astype(jnp.float32) + branch[frame]).astype(jnp.bfloat16)
            size = result.shape[0] // len(places)
            for n, (row, at) in enumerate(places):
                moved[frame, row + HALO, at, :] = result[n * size : (n + 1) * size]

    def fine_landed(slab):
        for shift in range(1, halves):
            fine_copy(shift, slab).wait_recv()

    def edge_step(step, carry):
        at = pl.ds(pl.multiple_of(step * thin, thin), thin)
        for group, when in enumerate((0, 1, 4)):

            @pl.when(step == when)
            def _():
                fine_landed(2 * group)
                fine_landed(2 * group + 1)

        motion_tile([(0, at), (rows - 1, at)])

        @pl.when(step == 0)
        def _():
            both(pl.ds(0, own), pl.ds(0, thin), 0, start, start)

        @pl.when(step > 0)
        def _():
            both(pl.ds(0, early), at, step, start, start)

        return carry

    def inner_step(step, carry):
        chunk, row = step // (rows - 2), 1 + lax.rem(step, rows - 2)
        for n in range(CHUNKS):

            @pl.when(step == n * (rows - 2))
            def _():
                mine_copy(2 * len(groups) + n).wait()
                fine_landed(2 * len(groups) + n)

        motion_tile([(row, pl.ds(pl.multiple_of(chunk * span, span), span))])
        return carry

    lax.fori_loop(0, STEPS, edge_step, 0)
    rest = pl.ds(thin, cols - thin)
    for frame in range(early, own):
        both(pl.ds(frame, 1), rest, STEPS + frame - early, start, start)
    lax.fori_loop(0, CHUNKS * (rows - 2), inner_step, 0)

    for copy in later_weights:
        copy.wait()

    def lifted(near, far):
        return jnp.dot(lift_ref[...], jnp.concatenate([near, far], axis=0), preferred_element_type=jnp.float32)

    def first_row(frame, r):
        first = conv_rows(x_ref.at[frame], r, 0, 3, cols, w1_ref)
        first = jnp.maximum(first, 0.0).astype(jnp.bfloat16).astype(jnp.float32)
        spread_columns(f_ref.at[frame], r, first, cols)

    def part_step(frame, carry):
        @pl.when(frame == 0)
        def _():
            landed(pl.ds(0, own), pl.ds(0, thin), 0)
            for step in range(1, STEPS):
                landed(pl.ds(0, early), pl.ds(step * thin, thin), step)

        @pl.when(frame >= early)
        def _():
            landed(pl.ds(frame, 1), rest, STEPS + frame - early)

        for r in range(rows + 2 * HALO):
            spread_columns(x_ref.at[frame], r, jnp.maximum(moved[frame, r].astype(jnp.float32), 0.0), cols)
        none = jnp.zeros_like(coarse[frame, 0])
        first_row(frame, rows - 1)
        part = conv_rows(f_ref.at[frame], rows - 1, 0, 1, cols, w2_ref) + lifted(none, coarse[frame, half - 1])
        part_out[0, frame] = part.astype(jnp.bfloat16)
        first_row(frame, 0)
        part = conv_rows(f_ref.at[frame], -2, 2, 3, cols, w2_ref) + lifted(none, coarse[frame, 0])
        part_out[1, frame] = part.astype(jnp.bfloat16)
        pl.when(has_after)(lambda: part_up(frame).start())
        pl.when(has_before)(lambda: part_down(frame).start())
        return carry

    def conv_step(frame, carry):
        for r in range(1, rows - 1):
            first_row(frame, r)
        for r in range(rows):
            near = coarse[frame, r // 2]
            none = jnp.zeros_like(near)
            if r == 0:
                far = jnp.where(has_before, none, near)
            elif r == rows - 1:
                far = jnp.where(has_after, none, near)
            else:
                far = coarse[frame, r // 2 - 1] if r % 2 == 0 else coarse[frame, r // 2 + 1]
            first_tap, last_tap = 1 if r == 0 else 0, 2 if r == rows - 1 else 3
            second = conv_rows(f_ref.at[frame], r - 1, first_tap, last_tap, cols, w2_ref)
            joined = lifted(near, far) + moved[frame, r + HALO].astype(jnp.float32) + second
            if r == 0:
                edges[frame, 0] = joined
            elif r == rows - 1:
                edges[frame, 1] = joined
            else:
                mine[frame, r] = joined.astype(jnp.bfloat16)
        return carry

    lax.fori_loop(0, own, part_step, 0)
    for shift in range(1, halves):
        for slab in range(len(slabs)):
            fine_copy(shift, slab).wait_send()
    lax.fori_loop(0, own, conv_step, 0)

    def join_step(frame, carry):
        pl.when(has_before)(lambda: part_up(frame).wait_recv())
        mine[frame, 0] = (edges[frame, 0] + part_in[0, frame].astype(jnp.float32)).astype(jnp.bfloat16)
        pl.when(has_after)(lambda: part_down(frame).wait_recv())
        mine[frame, rows - 1] = (edges[frame, 1] + part_in[1, frame].astype(jnp.float32)).astype(jnp.bfloat16)
        return carry

    lax.fori_loop(0, own, join_step, 0)
    for frame in range(own):
        pl.when(has_after)(lambda: part_up(frame).wait_send())
        pl.when(has_before)(lambda: part_down(frame).wait_send())
    both(pl.ds(0, own), pl.ds(0, thin), 0, wait_send, wait_send)
    for step in range(1, STEPS):
        both(pl.ds(0, early), pl.ds(step * thin, thin), step, wait_send, wait_send)
    for frame in range(early, own):
        both(pl.ds(frame, 1), rest, STEPS + frame - early, wait_send, wait_send)


def local(fine, coarse, w_query, w_key, w_value, w_out, conv_first, conv_second):
    own, rows, cols, width = fine.shape
    _, half, small, _ = coarse.shape
    bands, halves = lax.axis_size("space"), lax.axis_size("tm")
    pieces = STEPS + own - own // 2
    far = own * (halves - 1)
    slabs = 6 + CHUNKS
    any_space = pl.BlockSpec(memory_space=pl.ANY)
    bf16 = jnp.bfloat16
    pos = jnp.asarray(encode(own * halves, width))
    lift = jnp.asarray(lift_matrix(small))
    return pl.pallas_call(
        functools.partial(kernel, bands, halves),
        in_specs=[any_space] * 10,
        out_specs=pl.BlockSpec(memory_space=pltpu.VMEM),
        out_shape=pltpu.VMEM(fine.shape, bf16),
        scratch_shapes=[
            pltpu.VMEM((far, rows, cols, width), bf16),
            pltpu.VMEM((own, rows + 2 * HALO, cols, width), bf16),
            pltpu.VMEM((own, half, small, width), bf16),
            pltpu.VMEM((own, (rows + 2 * HALO) * cols, 3 * width), bf16),
            pltpu.VMEM((own, rows * cols, 3 * width), bf16),
            pltpu.VMEM(pos.shape, jnp.float32),
            pltpu.VMEM((width, width), bf16),
            pltpu.VMEM((width, width), bf16),
            pltpu.VMEM((width, width), bf16),
            pltpu.VMEM((width, width), bf16),
            pltpu.VMEM((9 * width, width), bf16),
            pltpu.VMEM((9 * width, width), bf16),
            pltpu.VMEM(lift.shape, bf16),
            pltpu.VMEM((own, 2, cols, width), jnp.float32),
            pltpu.VMEM((2, own, cols, width), bf16),
            pltpu.VMEM((2, own, cols, width), bf16),
            pltpu.SemaphoreType.DMA((9,)),
            pltpu.SemaphoreType.DMA((slabs,)),
            pltpu.SemaphoreType.DMA((halves - 1, slabs)),
            pltpu.SemaphoreType.DMA((halves - 1, slabs)),
            pltpu.SemaphoreType.DMA((2, pieces)),
            pltpu.SemaphoreType.DMA((2, pieces)),
            pltpu.SemaphoreType.DMA((2, own)),
            pltpu.SemaphoreType.DMA((2, own)),
        ],
        compiler_params=pltpu.CompilerParams(
            collective_id=0, has_side_effects=True, vmem_limit_bytes=54 * 1024 * 1024
        ),
        name="fused",
    )(
        fine, coarse, pos, w_query, w_key, w_value, w_out,
        conv_first.reshape(9 * width, width), conv_second.reshape(9 * width, width), lift,
    )


def solution(mesh):
    return jax.shard_map(
        local,
        mesh=mesh,
        in_specs=(
            P("tm", "space", None, None),
            P("tm", "space", None, None),
            P(),
            P(),
            P(),
            P(),
            P(),
            P(),
        ),
        out_specs=P("tm", "space", None, None),
        check_vma=False,
    )
```

```python
import functools

import jax
import jax.numpy as jnp
import numpy as np
from jax import lax
from jax.experimental import pallas as pl
from jax.experimental.pallas import tpu as pltpu
from jax.sharding import PartitionSpec as P

HEADS = 8
CHUNKS = 4
STEPS = 8
HALO = 1
LOG2E = 1.4426950408889634
MESH = pl.DeviceIdType.MESH


def encode(frames, width):
    half = width // 2
    inverse = np.exp(-np.log(10000.0) * 2.0 * np.arange(half) / width)
    angles = np.arange(frames)[:, None] * inverse[None, :]
    return np.concatenate([np.sin(angles), np.cos(angles)], axis=1).astype(np.float32)


def lift_matrix(small):
    out = np.arange(2 * small)[:, None]
    source = np.arange(small)[None, :]
    near = out // 2
    far = np.clip(np.where(out % 2 == 0, near - 1, near + 1), 0, small - 1)
    base = 0.75 * (source == near) + 0.25 * (source == far)
    return np.concatenate([0.75 * base, 0.25 * base], axis=1).astype(jnp.bfloat16)


def project(frames, own, pos, wq_ref, wk_ref, wv_ref, query_ref, key_ref, value_ref):
    tile, width = frames[0].shape
    scale = LOG2E / (float(width // HEADS) ** 0.5)
    normed = []
    for x, place in zip(frames, pos):
        hidden = x.astype(jnp.float32) + place
        center = hidden - jnp.mean(hidden, axis=-1, keepdims=True)
        spread = jnp.mean(center * center, axis=-1, keepdims=True)
        normed.append((center * lax.rsqrt(spread + 1e-05)).astype(jnp.bfloat16))
    flat = jnp.concatenate(normed, axis=0)
    query = jnp.dot(flat[: own * tile], wq_ref[...], preferred_element_type=jnp.float32)
    query_ref[...] = (query * scale).astype(jnp.bfloat16)
    key_ref[...] = jnp.dot(flat, wk_ref[...], preferred_element_type=jnp.float32).astype(jnp.bfloat16)
    value_ref[...] = jnp.dot(flat, wv_ref[...], preferred_element_type=jnp.float32).astype(jnp.bfloat16)


def iotas(rows, cols):
    return lax.broadcasted_iota(jnp.int32, (rows, cols), 0), lax.broadcasted_iota(jnp.int32, (rows, cols), 1)


def halve_heads(weight):
    width = weight.shape[1]
    depth = width // HEADS
    half = depth // 2
    source, place = iotas(width, width)
    side, lane = place // (width // 2), lax.rem(place, width // 2)
    wanted = lane // half * depth + side * half + lax.rem(lane, half)
    order = jnp.where(source == wanted, 1.0, 0.0).astype(jnp.bfloat16)
    return jnp.dot(weight, order, preferred_element_type=jnp.float32).astype(jnp.bfloat16)


def mix(tile, query_ref, key_ref, value_ref, wo_ref):
    size, width = query_ref.shape
    own, half = size // tile, width // 2
    query = query_ref[...].reshape(own, tile, width)
    source, place = iotas(2 * width, width)
    same_frame = source // width == place // half
    same_head = lax.rem(source, width) // (width // HEADS) == lax.rem(place, half) // (half // HEADS)
    blocks = jnp.where(same_frame & same_head, 1.0, 0.0).astype(jnp.bfloat16)
    places = [slice(at * tile, (at + 1) * tile) for at in range(key_ref.shape[0] // tile)]
    products = [(query * key_ref[at][None]).reshape(size, width) for at in places]
    scores = []
    for at in range(0, len(places), 2):
        pair = jnp.concatenate(products[at : at + 2], axis=1)
        pair = jnp.dot(pair, blocks, preferred_element_type=jnp.float32)
        scores += [pair[:, :half], pair[:, half:]]
    largest = functools.reduce(jnp.maximum, scores)
    total, summed = None, [None, None]
    for at, score in zip(places, scores):
        power = jnp.exp2(score - largest).reshape(own, tile, half)
        total = power if total is None else total + power
        for side in range(2):
            term = power * value_ref[at, side * half : (side + 1) * half].astype(jnp.float32)[None]
            summed[side] = term if summed[side] is None else summed[side] + term
    inverse = 1.0 / total
    attended = jnp.concatenate([(part * inverse).astype(jnp.bfloat16).reshape(size, half) for part in summed], axis=1)
    branch = jnp.dot(attended, wo_ref[...].reshape(width, width), preferred_element_type=jnp.float32)
    return branch.reshape(own, tile, width)


def spread_columns(ref, at, row, cols):
    column = lax.broadcasted_iota(jnp.int32, row.shape, 0)
    left = jnp.where(column == 0, 0.0, pltpu.roll(row, 1, 0))
    right = jnp.where(column == cols - 1, 0.0, pltpu.roll(row, cols - 1, 0))
    width = row.shape[1]
    ref[at * cols : (at + 1) * cols, :width] = left.astype(jnp.bfloat16)
    ref[at * cols : (at + 1) * cols, width : 2 * width] = row.astype(jnp.bfloat16)
    ref[at * cols : (at + 1) * cols, 2 * width :] = right.astype(jnp.bfloat16)


def conv_rows(ref, start, first, last, cols, weight_ref):
    pieces = [ref[(start + step) * cols : (start + step + 1) * cols, :] for step in range(first, last)]
    depth = ref.shape[1]
    return jnp.dot(
        jnp.concatenate(pieces, axis=1), weight_ref[first * depth : last * depth, :], preferred_element_type=jnp.float32
    )


def kernel(
    bands, halves, fine_ref, coarse_ref, pos_hbm, wq_hbm, wk_hbm, wv_hbm, wo_hbm, w1_hbm, w2_hbm, lift_hbm, mine,
    other, moved, coarse, x_ref, f_ref, pos_ref, wq_ref, wk_ref, wv_ref, wo_ref, w1_ref, w2_ref, lift_ref,
    edges, part_out, part_in, ring, query0, key0, value0, query1, key1, value1,
    weight_sems, local_sems, fine_send, fine_recv, halo_send, halo_recv, part_send, part_recv,
    ring_send, ring_recv, pass_send, pass_recv,
):
    own, rows, cols, width = mine.shape
    half = rows // 2
    span = cols // CHUNKS
    thin = cols // STEPS
    early = own // 2
    pieces = 2 * STEPS - 2
    groups = [(0, thin), (thin, thin), (2 * thin, 2 * thin), (4 * thin, cols - 4 * thin)]
    slabs = [(row, 1, at, size) for at, size in groups for row in (0, rows - 1)]
    slabs += [(1, rows - 2, chunk * span, span) for chunk in range(CHUNKS)]
    slots = ((query0, key0, value0), (query1, key1, value1))
    place, core = lax.axis_index("space"), lax.axis_index("tm")
    has_before, has_after = place > 0, place < bands - 1
    near_after = lax.rem(place, 2) == 0
    near_before = jnp.logical_not(near_after)

    def mine_copy(slab):
        row, count, at, size = slabs[slab]
        where = (slice(None), pl.ds(row, count), pl.ds(at, size))
        return pltpu.make_async_copy(fine_ref.at[where], mine.at[where], local_sems.at[slab])

    def fine_copy(shift, slab):
        row, count, at, size = slabs[slab]
        source = mine if count == 1 else fine_ref
        return pltpu.make_async_remote_copy(
            src_ref=source.at[:, pl.ds(row, count), pl.ds(at, size)],
            dst_ref=other.at[pl.ds((shift - 1) * own, own), pl.ds(row, count), pl.ds(at, size)],
            send_sem=fine_send.at[shift - 1, slab],
            recv_sem=fine_recv.at[shift - 1, slab],
            device_id={"tm": lax.rem(core + halves - shift, halves)},
            device_id_type=MESH,
        )

    def to_after(src, dst, send, recv):
        return pltpu.make_async_remote_copy(
            src_ref=src, dst_ref=dst, send_sem=send, recv_sem=recv, device_id={"space": place + 1}, device_id_type=MESH
        )

    def to_before(src, dst, send, recv):
        return pltpu.make_async_remote_copy(
            src_ref=src, dst_ref=dst, send_sem=send, recv_sem=recv, device_id={"space": place - 1}, device_id_type=MESH
        )

    def part_up(frame):
        return to_after(part_out.at[0, frame], part_in.at[0, frame], part_send.at[0, frame], part_recv.at[0, frame])

    def part_down(frame):
        return to_before(part_out.at[1, frame], part_in.at[1, frame], part_send.at[1, frame], part_recv.at[1, frame])

    def ring_up():
        return to_after(mine.at[:, rows - 1, 0:thin], ring.at[0, 0:own], ring_send.at[0], ring_recv.at[0])

    def ring_down():
        return to_before(mine.at[:, 0, 0:thin], ring.at[1, 0:own], ring_send.at[1], ring_recv.at[1])

    def ring_pass(shift):
        return pltpu.make_async_remote_copy(
            src_ref=ring.at[:, 0:own],
            dst_ref=ring.at[:, pl.ds(shift * own, own)],
            send_sem=pass_send.at[shift - 1],
            recv_sem=pass_recv.at[shift - 1],
            device_id={"tm": lax.rem(core + halves - shift, halves)},
            device_id_type=MESH,
        )

    def halo_up(frames, span_at, piece):
        return to_after(
            moved.at[frames, rows : rows + HALO, span_at], moved.at[frames, 0:HALO, span_at],
            halo_send.at[0, piece], halo_recv.at[0, piece],
        )

    def halo_down(frames, span_at, piece):
        return to_before(
            moved.at[frames, HALO : 2 * HALO, span_at], moved.at[frames, rows + HALO : rows + 2 * HALO, span_at],
            halo_send.at[1, piece], halo_recv.at[1, piece],
        )

    def start(copy):
        copy.start()

    def wait_send(copy):
        copy.wait_send()

    def piece(at, act, up_if, down_if):
        for first, low, high in ((0, 0, early), (STEPS - 1, early, own)):

            @pl.when((at >= first) & (at < first + STEPS - 1))
            def _():
                columns = pl.ds(pl.multiple_of((at - first + 1) * thin, thin), thin)
                frames = pl.ds(low, high - low)
                pl.when(up_if)(lambda: act(halo_up(frames, columns, at)))
                pl.when(down_if)(lambda: act(halo_down(frames, columns, at)))

    def each_piece(low, high, act, up_if, down_if):
        lax.fori_loop(low, high, lambda at, carry: (piece(at, act, up_if, down_if), carry)[1], 0)

    def wait_recv(copy):
        copy.wait_recv()

    def landed(low, high):
        each_piece(low, high, wait_recv, has_before, has_after)

    barrier = pltpu.get_barrier_semaphore()
    for shift in range(1, halves):
        pl.semaphore_signal(barrier, inc=1, device_id={"tm": lax.rem(core + shift, halves)}, device_id_type=MESH)

    @pl.when(has_before)
    def _():
        pl.semaphore_signal(barrier, inc=1, device_id={"space": place - 1}, device_id_type=MESH)

    @pl.when(has_after)
    def _():
        pl.semaphore_signal(barrier, inc=1, device_id={"space": place + 1}, device_id_type=MESH)

    motion_weights = [
        pltpu.make_async_copy(src, dst, weight_sems.at[at])
        for at, (src, dst) in enumerate(
            [(wv_hbm, wv_ref), (pos_hbm, pos_ref), (wq_hbm, wq_ref), (wk_hbm, wk_ref)]
            + [(wo_hbm.at[:, side], wo_ref.at[side]) for side in range(2)]
        )
    ]
    later_weights = [
        pltpu.make_async_copy(src, dst, weight_sems.at[6 + at])
        for at, (src, dst) in enumerate(
            [(lift_hbm, lift_ref), (w1_hbm, w1_ref), (w2_hbm, w2_ref), (coarse_ref, coarse)]
        )
    ]
    for slab in range(4):
        mine_copy(slab).start()
    for copy in motion_weights:
        copy.start()
    for slab in range(4, len(slabs)):
        mine_copy(slab).start()
    for copy in later_weights:
        copy.start()

    @pl.when(jnp.logical_not(has_before))
    def _():
        moved[:, 0:HALO] = jnp.zeros((own, HALO, cols, width), jnp.bfloat16)
        part_in[0] = jnp.zeros((own, cols, width), jnp.bfloat16)
        ring[0, 0:own] = jnp.zeros((own, thin, width), jnp.bfloat16)

    @pl.when(jnp.logical_not(has_after))
    def _():
        moved[:, rows + HALO :] = jnp.zeros((own, HALO, cols, width), jnp.bfloat16)
        part_in[1] = jnp.zeros((own, cols, width), jnp.bfloat16)
        ring[1, 0:own] = jnp.zeros((own, thin, width), jnp.bfloat16)

    motion_weights[0].wait()
    wv_ref[...] = halve_heads(wv_ref[...])
    peers = halves - 1 + has_before.astype(jnp.int32) + has_after.astype(jnp.int32)
    pl.semaphore_wait(barrier, peers)

    mine_copy(0).wait()
    mine_copy(1).wait()
    pl.when(has_after)(lambda: ring_up().start())
    pl.when(has_before)(lambda: ring_down().start())
    for slab in (2, 3, 4, 5, 6, 7, 0, 1, *range(8, len(slabs))):
        if 2 <= slab < 8:
            mine_copy(slab).wait()
        for shift in range(1, halves):
            fine_copy(shift, slab).start()
    for copy in motion_weights[1:]:
        copy.wait()

    pos = []
    for shift in range(halves):
        for frame in range(own):
            pos.append(pos_ref[pl.ds(lax.rem(core + shift, halves) * own + frame, 1), :])

    def fine_landed(slab):
        for shift in range(1, halves):
            fine_copy(shift, slab).wait_recv()

    needs = {0: (2, 3), 1: (4, 5), 3: (6, 7), STEPS - 1: (0, 1)}
    for chunk in range(CHUNKS):
        needs[STEPS + max(chunk * STEPS // CHUNKS - 1, 0)] = (2 * len(groups) + chunk,)

    def places_of(tile):
        pair, step = tile // STEPS, lax.rem(tile + 1, STEPS)
        at = pl.ds(pl.multiple_of(step * thin, thin), thin)
        return (pair, at), (rows - 1 - pair, at)

    def arrive(tile):
        for when, waits in needs.items():

            @pl.when(tile == when)
            def _():
                for slab in waits:
                    if slabs[slab][1] > 1:
                        mine_copy(slab).wait()
                    fine_landed(slab)

        pl.when(tile == STEPS - 2)(pass_ring)

    def pass_ring():
        pl.when(has_before)(lambda: ring_up().wait_recv())
        pl.when(has_after)(lambda: ring_down().wait_recv())
        for shift in range(1, halves):
            ring_pass(shift).start()

    def enter_ring(slot):
        frames = [jnp.concatenate([ring[0, frame], ring[1, frame]]) for frame in range(own * halves)]
        project(frames, own, pos, wq_ref, wk_ref, wv_ref, *slots[slot])

    def leave_ring(slot):
        branch = mix(2 * thin, *slots[slot], wo_ref)
        for frame in range(own):
            for side, real in enumerate((has_before, has_after)):
                result = ring[side, frame].astype(jnp.float32) + branch[frame, side * thin : (side + 1) * thin]
                moved[frame, side * (rows + HALO), 0:thin, :] = jnp.where(real, result, 0.0).astype(jnp.bfloat16)

    def enter(tile, slot):
        places = places_of(tile)
        frames = [jnp.concatenate([mine[frame, row, at, :] for row, at in places]) for frame in range(own)]
        frames += [
            jnp.concatenate([other[frame, row, at, :] for row, at in places]) for frame in range(own * (halves - 1))
        ]
        project(frames, own, pos, wq_ref, wk_ref, wv_ref, *slots[slot])

    def leave(tile, slot):
        places = places_of(tile)
        branch = mix(2 * thin, *slots[slot], wo_ref)
        for frame in range(own):
            for n, (row, at) in enumerate(places):
                result = mine[frame, row, at, :].astype(jnp.float32) + branch[frame, n * thin : (n + 1) * thin]
                moved[frame, row + HALO, at, :] = result.astype(jnp.bfloat16)

    def hand_over(tile):
        now = tile < STEPS - 1
        piece(tile, start, has_after & (now | near_after), has_before & (now | near_before))

    def turn(tile, slot):
        arrive(tile + 1)
        leave(tile, slot)
        enter(tile + 1, 1 - slot)
        hand_over(tile)

    def two_turns(step, carry):
        turn(2 * step, 0)
        turn(2 * step + 1, 1)
        return carry

    tiles = STEPS * (rows // 2)
    arrive(0)
    enter(0, 0)
    lax.fori_loop(0, tiles // 2 - 1, two_turns, 0)
    turn(tiles - 2, 0)
    for shift in range(1, halves):
        ring_pass(shift).wait_recv()
    leave(tiles - 1, 1)
    enter_ring(0)
    each_piece(STEPS - 1, pieces, start, has_after & near_before, has_before & near_after)
    each_piece(tiles - 1, pieces, start, has_after & near_after, has_before & near_before)
    leave_ring(0)

    for copy in later_weights:
        copy.wait()

    def lifted(near, far):
        return jnp.dot(lift_ref[...], jnp.concatenate([near, far], axis=0), preferred_element_type=jnp.float32)

    def first_row(frame, r):
        first = conv_rows(x_ref.at[frame], r, 0, 3, cols, w1_ref)
        first = jnp.maximum(first, 0.0).astype(jnp.bfloat16).astype(jnp.float32)
        spread_columns(f_ref.at[frame], r, first, cols)

    def part_step(frame):
        pl.when(frame == 0)(lambda: landed(0, STEPS - 1))
        for r in range(rows + 2 * HALO):
            spread_columns(x_ref.at[frame], r, jnp.maximum(moved[frame, r].astype(jnp.float32), 0.0), cols)
        none = jnp.zeros_like(coarse[frame, 0])
        first_row(frame, rows - 1)
        part = conv_rows(f_ref.at[frame], rows - 1, 0, 1, cols, w2_ref) + lifted(none, coarse[frame, half - 1])
        part_out[0, frame] = part.astype(jnp.bfloat16)
        first_row(frame, 0)
        part = conv_rows(f_ref.at[frame], -2, 2, 3, cols, w2_ref) + lifted(none, coarse[frame, 0])
        part_out[1, frame] = part.astype(jnp.bfloat16)
        now = frame > 1
        pl.when(has_after & (now | near_after))(lambda: part_up(frame).start())
        pl.when(has_before & (now | near_before))(lambda: part_down(frame).start())

    def held_parts():
        landed(STEPS - 1, pieces)
        for frame in range(2):
            pl.when(has_after & near_before)(lambda: part_up(frame).start())
            pl.when(has_before & near_after)(lambda: part_down(frame).start())

    def conv_step(frame):
        for r in range(1, rows - 1):
            first_row(frame, r)
        for r in range(rows):
            near = coarse[frame, r // 2]
            none = jnp.zeros_like(near)
            if r == 0:
                far = jnp.where(has_before, none, near)
            elif r == rows - 1:
                far = jnp.where(has_after, none, near)
            else:
                far = coarse[frame, r // 2 - 1] if r % 2 == 0 else coarse[frame, r // 2 + 1]
            first_tap, last_tap = 1 if r == 0 else 0, 2 if r == rows - 1 else 3
            second = conv_rows(f_ref.at[frame], r - 1, first_tap, last_tap, cols, w2_ref)
            joined = lifted(near, far) + moved[frame, r + HALO].astype(jnp.float32) + second
            if r == 0:
                edges[frame, 0] = joined
            elif r == rows - 1:
                edges[frame, 1] = joined
            else:
                mine[frame, r] = joined.astype(jnp.bfloat16)

    def conv_turn(turn, carry):
        pl.when(turn >= 2)(lambda: conv_step(turn - 2))
        pl.when(turn == 2)(held_parts)
        pl.when(turn < own)(lambda: part_step(turn))
        return carry

    for shift in range(1, halves):
        for slab in range(len(slabs)):
            fine_copy(shift, slab).wait_send()
    lax.fori_loop(0, own + 2, conv_turn, 0)

    each_piece(0, pieces, wait_send, has_after, has_before)
    pl.when(has_after)(lambda: ring_up().wait_send())
    pl.when(has_before)(lambda: ring_down().wait_send())
    for shift in range(1, halves):
        ring_pass(shift).wait_send()

    def join_step(frame, carry):
        pl.when(has_after)(lambda: part_up(frame).wait_send())
        pl.when(has_before)(lambda: part_down(frame).wait_send())
        pl.when(has_before)(lambda: part_up(frame).wait_recv())
        mine[frame, 0] = (edges[frame, 0] + part_in[0, frame].astype(jnp.float32)).astype(jnp.bfloat16)
        pl.when(has_after)(lambda: part_down(frame).wait_recv())
        mine[frame, rows - 1] = (edges[frame, 1] + part_in[1, frame].astype(jnp.float32)).astype(jnp.bfloat16)
        return carry

    lax.fori_loop(0, own, join_step, 0)


def local(fine, coarse, w_query, w_key, w_value, w_out, conv_first, conv_second):
    own, rows, cols, width = fine.shape
    _, half, small, _ = coarse.shape
    bands, halves = lax.axis_size("space"), lax.axis_size("tm")
    pieces = 2 * STEPS - 2
    far = own * (halves - 1)
    slabs = 8 + CHUNKS
    halved = (2, HEADS, width // HEADS // 2, width)
    any_space = pl.BlockSpec(memory_space=pl.ANY)
    bf16 = jnp.bfloat16
    pos = jnp.asarray(encode(own * halves, width))
    lift = jnp.asarray(lift_matrix(small))
    return pl.pallas_call(
        functools.partial(kernel, bands, halves),
        in_specs=[any_space] * 10,
        out_specs=pl.BlockSpec(memory_space=pltpu.VMEM),
        out_shape=pltpu.VMEM(fine.shape, bf16),
        scratch_shapes=[
            pltpu.VMEM((far, rows, cols, width), bf16),
            pltpu.VMEM((own, rows + 2 * HALO, cols, width), bf16),
            pltpu.VMEM((own, half, small, width), bf16),
            pltpu.VMEM((own, (rows + 2 * HALO) * cols, 3 * width), bf16),
            pltpu.VMEM((own, rows * cols, 3 * width), bf16),
            pltpu.VMEM(pos.shape, jnp.float32),
            pltpu.VMEM((width, width), bf16),
            pltpu.VMEM((width, width), bf16),
            pltpu.VMEM((width, width), bf16),
            pltpu.VMEM(halved, bf16),
            pltpu.VMEM((9 * width, width), bf16),
            pltpu.VMEM((9 * width, width), bf16),
            pltpu.VMEM(lift.shape, bf16),
            pltpu.VMEM((own, 2, cols, width), jnp.float32),
            pltpu.VMEM((2, own, cols, width), bf16),
            pltpu.VMEM((2, own, cols, width), bf16),
            pltpu.VMEM((2, own * halves, cols // STEPS, width), bf16),
            *[pltpu.VMEM((count * 2 * cols // STEPS, width), bf16) for count in (own, own + far, own + far)] * 2,
            pltpu.SemaphoreType.DMA((10,)),
            pltpu.SemaphoreType.DMA((slabs,)),
            pltpu.SemaphoreType.DMA((halves - 1, slabs)),
            pltpu.SemaphoreType.DMA((halves - 1, slabs)),
            pltpu.SemaphoreType.DMA((2, pieces)),
            pltpu.SemaphoreType.DMA((2, pieces)),
            pltpu.SemaphoreType.DMA((2, own)),
            pltpu.SemaphoreType.DMA((2, own)),
            pltpu.SemaphoreType.DMA((2,)),
            pltpu.SemaphoreType.DMA((2,)),
            pltpu.SemaphoreType.DMA((halves - 1,)),
            pltpu.SemaphoreType.DMA((halves - 1,)),
        ],
        compiler_params=pltpu.CompilerParams(
            collective_id=0, has_side_effects=True, vmem_limit_bytes=54 * 1024 * 1024
        ),
        name="fused",
    )(
        fine, coarse, pos, w_query, w_key, w_value,
        w_out.reshape(HEADS, 2, width // HEADS // 2, width), conv_first.reshape(9 * width, width), conv_second.reshape(9 * width, width), lift,
    )


def solution(mesh):
    return jax.shard_map(
        local,
        mesh=mesh,
        in_specs=(
            P("tm", "space", None, None),
            P("tm", "space", None, None),
            P(),
            P(),
            P(),
            P(),
            P(),
            P(),
        ),
        out_specs=P("tm", "space", None, None),
        check_vma=False,
    )
```

```python
import functools

import jax
import jax.numpy as jnp
import numpy as np
from jax import lax
from jax.experimental import pallas as pl
from jax.experimental.pallas import tpu as pltpu
from jax.sharding import PartitionSpec as P

HEADS = 8
CHUNKS = 4
STEPS = 8
HALO = 1
LOG2E = 1.4426950408889634
MESH = pl.DeviceIdType.MESH


def encode(frames, width):
    half = width // 2
    inverse = np.exp(-np.log(10000.0) * 2.0 * np.arange(half) / width)
    angles = np.arange(frames)[:, None] * inverse[None, :]
    return np.concatenate([np.sin(angles), np.cos(angles)], axis=1).astype(np.float32)


def lift_matrix(small):
    out = np.arange(2 * small)[:, None]
    source = np.arange(small)[None, :]
    near = out // 2
    far = np.clip(np.where(out % 2 == 0, near - 1, near + 1), 0, small - 1)
    base = 0.75 * (source == near) + 0.25 * (source == far)
    return np.concatenate([0.75 * base, 0.25 * base], axis=1).astype(jnp.bfloat16)


def project(frames, own, pos, wq_ref, wk_ref, wv_ref, query_ref, key_ref, value_ref):
    tile, width = frames[0].shape
    scale = LOG2E / (float(width // HEADS) ** 0.5)
    normed = []
    for x, place in zip(frames, pos):
        hidden = x.astype(jnp.float32) + place
        center = hidden - jnp.mean(hidden, axis=-1, keepdims=True)
        spread = jnp.mean(center * center, axis=-1, keepdims=True)
        normed.append((center * lax.rsqrt(spread + 1e-05)).astype(jnp.bfloat16))
    flat = jnp.concatenate(normed, axis=0)
    query = jnp.dot(flat[: own * tile], wq_ref[...], preferred_element_type=jnp.float32)
    query_ref[...] = (query * scale).astype(jnp.bfloat16)
    key_ref[...] = jnp.dot(flat, wk_ref[...], preferred_element_type=jnp.float32).astype(jnp.bfloat16)
    value_ref[...] = jnp.dot(flat, wv_ref[...], preferred_element_type=jnp.float32).astype(jnp.bfloat16)


def iotas(rows, cols):
    return lax.broadcasted_iota(jnp.int32, (rows, cols), 0), lax.broadcasted_iota(jnp.int32, (rows, cols), 1)


def halve_heads(weight):
    width = weight.shape[1]
    depth = width // HEADS
    half = depth // 2
    source, place = iotas(width, width)
    side, lane = place // (width // 2), lax.rem(place, width // 2)
    wanted = lane // half * depth + side * half + lax.rem(lane, half)
    order = jnp.where(source == wanted, 1.0, 0.0).astype(jnp.bfloat16)
    return jnp.dot(weight, order, preferred_element_type=jnp.float32).astype(jnp.bfloat16)


def mix(tile, query_ref, key_ref, value_ref, wo_ref):
    size, width = query_ref.shape
    own, half = size // tile, width // 2
    query = query_ref[...].reshape(own, tile, width)
    source, place = iotas(2 * width, width)
    same_frame = source // width == place // half
    same_head = lax.rem(source, width) // (width // HEADS) == lax.rem(place, half) // (half // HEADS)
    blocks = jnp.where(same_frame & same_head, 1.0, 0.0).astype(jnp.bfloat16)
    places = [slice(at * tile, (at + 1) * tile) for at in range(key_ref.shape[0] // tile)]
    products = [(query * key_ref[at][None]).reshape(size, width) for at in places]
    scores = []
    for at in range(0, len(places), 2):
        pair = jnp.concatenate(products[at : at + 2], axis=1)
        pair = jnp.dot(pair, blocks, preferred_element_type=jnp.float32)
        scores += [pair[:, :half], pair[:, half:]]
    largest = functools.reduce(jnp.maximum, scores)
    total, summed = None, [None, None]
    for at, score in zip(places, scores):
        power = jnp.exp2(score - largest).reshape(own, tile, half)
        total = power if total is None else total + power
        for side in range(2):
            term = power * value_ref[at, side * half : (side + 1) * half].astype(jnp.float32)[None]
            summed[side] = term if summed[side] is None else summed[side] + term
    inverse = 1.0 / total
    attended = jnp.concatenate([(part * inverse).astype(jnp.bfloat16).reshape(size, half) for part in summed], axis=1)
    branch = jnp.dot(attended, wo_ref[...].reshape(width, width), preferred_element_type=jnp.float32)
    return branch.reshape(own, tile, width)


def spread_columns(ref, at, row, cols):
    column = lax.broadcasted_iota(jnp.int32, row.shape, 0)
    left = jnp.where(column == 0, 0.0, pltpu.roll(row, 1, 0))
    right = jnp.where(column == cols - 1, 0.0, pltpu.roll(row, cols - 1, 0))
    width = row.shape[1]
    ref[at * cols : (at + 1) * cols, :width] = left.astype(jnp.bfloat16)
    ref[at * cols : (at + 1) * cols, width : 2 * width] = row.astype(jnp.bfloat16)
    ref[at * cols : (at + 1) * cols, 2 * width :] = right.astype(jnp.bfloat16)


def conv_rows(ref, start, first, last, cols, weight_ref):
    pieces = [ref[(start + step) * cols : (start + step + 1) * cols, :] for step in range(first, last)]
    depth = ref.shape[1]
    return jnp.dot(
        jnp.concatenate(pieces, axis=1), weight_ref[first * depth : last * depth, :], preferred_element_type=jnp.float32
    )


def kernel(
    bands, halves, fine_ref, coarse_ref, pos_hbm, wq_hbm, wk_hbm, wv_hbm, wo_hbm, w1_hbm, w2_hbm, lift_hbm, mine,
    other, moved, coarse, x_ref, f_ref, pos_ref, wq_ref, wk_ref, wv_ref, wo_ref, w1_ref, w2_ref, lift_ref,
    edges, part_out, part_in, ring, query0, key0, value0, query1, key1, value1,
    weight_sems, local_sems, fine_send, fine_recv, halo_send, halo_recv, part_send, part_recv,
    ring_send, ring_recv, pass_send, pass_recv,
):
    own, rows, cols, width = mine.shape
    half = rows // 2
    span = cols // CHUNKS
    thin = cols // STEPS
    early = own // 2
    pieces = 2 * STEPS - 2
    groups = [(0, thin), (thin, thin), (2 * thin, 2 * thin), (4 * thin, cols - 4 * thin)]
    slabs = [(row, 1, at, size) for at, size in groups for row in (0, rows - 1)]
    slabs += [(1, rows - 2, chunk * span, span) for chunk in range(CHUNKS)]
    lots = [slab // 2 if slab < 2 * len(groups) else slab - len(groups) for slab in range(len(slabs))]
    slots = ((query0, key0, value0), (query1, key1, value1))
    place, core = lax.axis_index("space"), lax.axis_index("tm")
    has_before, has_after = place > 0, place < bands - 1
    near_after = lax.rem(place, 2) == 0
    near_before = jnp.logical_not(near_after)

    def mine_copy(slab):
        row, count, at, size = slabs[slab]
        where = (slice(None), pl.ds(row, count), pl.ds(at, size))
        return pltpu.make_async_copy(fine_ref.at[where], mine.at[where], local_sems.at[lots[slab]])

    def fine_copy(shift, slab):
        row, count, at, size = slabs[slab]
        source = mine if count == 1 else fine_ref
        return pltpu.make_async_remote_copy(
            src_ref=source.at[:, pl.ds(row, count), pl.ds(at, size)],
            dst_ref=other.at[pl.ds((shift - 1) * own, own), pl.ds(row, count), pl.ds(at, size)],
            send_sem=fine_send.at[shift - 1],
            recv_sem=fine_recv.at[shift - 1, lots[slab]],
            device_id={"tm": lax.rem(core + halves - shift, halves)},
            device_id_type=MESH,
        )

    def lot_part(lot):
        if lot < len(groups):
            return (slice(None), pl.ds(0, 2), pl.ds(*groups[lot]))
        row, count, at, size = slabs[lot + len(groups)]
        return (slice(None), pl.ds(row, count), pl.ds(at, size))

    def mine_landed(lot):
        where = lot_part(lot)
        pltpu.make_async_copy(fine_ref.at[where], mine.at[where], local_sems.at[lot]).wait()

    def fine_landed(lot):
        where = lot_part(lot)
        for shift in range(1, halves):
            pltpu.make_async_remote_copy(
                src_ref=mine.at[where],
                dst_ref=other.at[pl.ds((shift - 1) * own, own), *where[1:]],
                send_sem=fine_send.at[shift - 1],
                recv_sem=fine_recv.at[shift - 1, lot],
                device_id={"tm": lax.rem(core + halves - shift, halves)},
                device_id_type=MESH,
            ).wait_recv()

    def fine_left():
        for shift in range(1, halves):
            pltpu.make_async_remote_copy(
                src_ref=mine,
                dst_ref=other.at[pl.ds((shift - 1) * own, own)],
                send_sem=fine_send.at[shift - 1],
                recv_sem=fine_recv.at[shift - 1, 0],
                device_id={"tm": lax.rem(core + halves - shift, halves)},
                device_id_type=MESH,
            ).wait_send()

    def to_after(src, dst, send, recv):
        return pltpu.make_async_remote_copy(
            src_ref=src, dst_ref=dst, send_sem=send, recv_sem=recv, device_id={"space": place + 1}, device_id_type=MESH
        )

    def to_before(src, dst, send, recv):
        return pltpu.make_async_remote_copy(
            src_ref=src, dst_ref=dst, send_sem=send, recv_sem=recv, device_id={"space": place - 1}, device_id_type=MESH
        )

    def part_up(frame):
        return to_after(part_out.at[0, frame], part_in.at[0, frame], part_send.at[0], part_recv.at[0, frame])

    def part_down(frame):
        return to_before(part_out.at[1, frame], part_in.at[1, frame], part_send.at[1], part_recv.at[1, frame])

    def ring_up():
        return to_after(mine.at[:, rows - 1, 0:thin], ring.at[0, 0:own], ring_send.at[0], ring_recv.at[0])

    def ring_down():
        return to_before(mine.at[:, 0, 0:thin], ring.at[1, 0:own], ring_send.at[1], ring_recv.at[1])

    def ring_pass(shift):
        return pltpu.make_async_remote_copy(
            src_ref=ring.at[:, 0:own],
            dst_ref=ring.at[:, pl.ds(shift * own, own)],
            send_sem=pass_send.at[shift - 1],
            recv_sem=pass_recv.at[shift - 1],
            device_id={"tm": lax.rem(core + halves - shift, halves)},
            device_id_type=MESH,
        )

    def halo_up(frames, span_at, late):
        return to_after(
            moved.at[frames, rows : rows + HALO, span_at], moved.at[frames, 0:HALO, span_at],
            halo_send.at[0], halo_recv.at[0, late],
        )

    def halo_down(frames, span_at, late):
        return to_before(
            moved.at[frames, HALO : 2 * HALO, span_at], moved.at[frames, rows + HALO : rows + 2 * HALO, span_at],
            halo_send.at[1], halo_recv.at[1, late],
        )

    crowd = ((0, early), (early, own - early), (0, own))

    def piece(at, up_if, down_if):
        for late in range(2):

            @pl.when((at >= late * (STEPS - 1)) & (at < (late + 1) * (STEPS - 1)))
            def _():
                columns = pl.ds(pl.multiple_of((at - late * (STEPS - 1) + 1) * thin, thin), thin)
                frames = pl.ds(*crowd[late])
                pl.when(up_if)(lambda: halo_up(frames, columns, late).start())
                pl.when(down_if)(lambda: halo_down(frames, columns, late).start())

    def each_piece(low, high, up_if, down_if):
        lax.fori_loop(low, high, lambda at, carry: (piece(at, up_if, down_if), carry)[1], 0)

    def landed(late):
        frames = pl.ds(*crowd[late])
        pl.when(has_before)(lambda: halo_up(frames, rest, late).wait_recv())
        pl.when(has_after)(lambda: halo_down(frames, rest, late).wait_recv())

    rest = pl.ds(thin, cols - thin)
    barrier = pltpu.get_barrier_semaphore()
    for shift in range(1, halves):
        pl.semaphore_signal(barrier, inc=1, device_id={"tm": lax.rem(core + shift, halves)}, device_id_type=MESH)

    @pl.when(has_before)
    def _():
        pl.semaphore_signal(barrier, inc=1, device_id={"space": place - 1}, device_id_type=MESH)

    @pl.when(has_after)
    def _():
        pl.semaphore_signal(barrier, inc=1, device_id={"space": place + 1}, device_id_type=MESH)

    motion_weights = [
        pltpu.make_async_copy(src, dst, weight_sems.at[at])
        for at, (src, dst) in enumerate(
            [(wv_hbm, wv_ref), (pos_hbm, pos_ref), (wq_hbm, wq_ref), (wk_hbm, wk_ref)]
            + [(wo_hbm.at[:, side], wo_ref.at[side]) for side in range(2)]
        )
    ]
    later_weights = [
        pltpu.make_async_copy(src, dst, weight_sems.at[6 + at])
        for at, (src, dst) in enumerate(
            [(lift_hbm, lift_ref), (w1_hbm, w1_ref), (w2_hbm, w2_ref), (coarse_ref, coarse)]
        )
    ]
    for slab in range(4):
        mine_copy(slab).start()
    for copy in motion_weights:
        copy.start()
    for slab in range(4, len(slabs)):
        mine_copy(slab).start()
    for copy in later_weights:
        copy.start()

    @pl.when(jnp.logical_not(has_before))
    def _():
        moved[:, 0:HALO] = jnp.zeros((own, HALO, cols, width), jnp.bfloat16)
        part_in[0] = jnp.zeros((own, cols, width), jnp.bfloat16)
        ring[0, 0:own] = jnp.zeros((own, thin, width), jnp.bfloat16)

    @pl.when(jnp.logical_not(has_after))
    def _():
        moved[:, rows + HALO :] = jnp.zeros((own, HALO, cols, width), jnp.bfloat16)
        part_in[1] = jnp.zeros((own, cols, width), jnp.bfloat16)
        ring[1, 0:own] = jnp.zeros((own, thin, width), jnp.bfloat16)

    peers = halves - 1 + has_before.astype(jnp.int32) + has_after.astype(jnp.int32)
    pl.semaphore_wait(barrier, peers)

    mine_landed(0)
    pl.when(has_after)(lambda: ring_up().start())
    pl.when(has_before)(lambda: ring_down().start())
    for slab in (2, 3, 4, 5, 6, 7, 0, 1, *range(8, len(slabs))):
        if slab in (2, 4, 6):
            mine_landed(lots[slab])
        for shift in range(1, halves):
            fine_copy(shift, slab).start()
    motion_weights[0].wait()
    wv_ref[...] = halve_heads(wv_ref[...])
    for copy in motion_weights[1:]:
        copy.wait()

    pos = []
    for shift in range(halves):
        for frame in range(own):
            pos.append(pos_ref[pl.ds(lax.rem(core + shift, halves) * own + frame, 1), :])

    needs = {0: 1, 1: 2, 3: 3, STEPS - 1: 0}
    for chunk in range(CHUNKS):
        needs[STEPS + max(chunk * STEPS // CHUNKS - 1, 0)] = len(groups) + chunk

    def places_of(tile):
        pair, step = tile // STEPS, lax.rem(tile + 1, STEPS)
        at = pl.ds(pl.multiple_of(step * thin, thin), thin)
        return (pair, at), (rows - 1 - pair, at)

    def arrive(tile):
        for when, lot in needs.items():

            @pl.when(tile == when)
            def _():
                if lot >= len(groups):
                    mine_landed(lot)
                fine_landed(lot)

        pl.when(tile == STEPS - 2)(pass_ring)

    def pass_ring():
        pl.when(has_before)(lambda: ring_up().wait_recv())
        pl.when(has_after)(lambda: ring_down().wait_recv())
        for shift in range(1, halves):
            ring_pass(shift).start()

    def enter_ring(slot):
        frames = [jnp.concatenate([ring[0, frame], ring[1, frame]]) for frame in range(own * halves)]
        project(frames, own, pos, wq_ref, wk_ref, wv_ref, *slots[slot])

    def leave_ring(slot):
        branch = mix(2 * thin, *slots[slot], wo_ref)
        for frame in range(own):
            for side, real in enumerate((has_before, has_after)):
                result = ring[side, frame].astype(jnp.float32) + branch[frame, side * thin : (side + 1) * thin]
                moved[frame, side * (rows + HALO), 0:thin, :] = jnp.where(real, result, 0.0).astype(jnp.bfloat16)

    def enter(tile, slot):
        places = places_of(tile)
        frames = [jnp.concatenate([mine[frame, row, at, :] for row, at in places]) for frame in range(own)]
        frames += [
            jnp.concatenate([other[frame, row, at, :] for row, at in places]) for frame in range(own * (halves - 1))
        ]
        project(frames, own, pos, wq_ref, wk_ref, wv_ref, *slots[slot])

    def leave(tile, slot):
        places = places_of(tile)
        branch = mix(2 * thin, *slots[slot], wo_ref)
        for frame in range(own):
            for n, (row, at) in enumerate(places):
                result = mine[frame, row, at, :].astype(jnp.float32) + branch[frame, n * thin : (n + 1) * thin]
                moved[frame, row + HALO, at, :] = result.astype(jnp.bfloat16)

    def hand_over(tile):
        now = tile < STEPS - 1
        piece(tile, has_after & (now | near_after), has_before & (now | near_before))

        @pl.when(tile == 12)
        def _():
            each_piece(STEPS - 1, pieces, has_after & near_before, has_before & near_after)

    def turn(tile, slot):
        arrive(tile + 1)
        leave(tile, slot)
        enter(tile + 1, 1 - slot)
        hand_over(tile)

    def two_turns(step, carry):
        turn(2 * step, 0)
        turn(2 * step + 1, 1)
        return carry

    tiles = STEPS * (rows // 2)
    arrive(0)
    enter(0, 0)
    lax.fori_loop(0, tiles // 2 - 1, two_turns, 0)
    turn(tiles - 2, 0)
    for shift in range(1, halves):
        ring_pass(shift).wait_recv()
    leave(tiles - 1, 1)
    enter_ring(0)
    each_piece(tiles - 1, pieces, has_after & near_after, has_before & near_before)
    leave_ring(0)

    for copy in later_weights:
        copy.wait()

    def lifted(near, far):
        return jnp.dot(lift_ref[...], jnp.concatenate([near, far], axis=0), preferred_element_type=jnp.float32)

    def first_row(frame, r):
        first = conv_rows(x_ref.at[frame], r, 0, 3, cols, w1_ref)
        first = jnp.maximum(first, 0.0).astype(jnp.bfloat16).astype(jnp.float32)
        spread_columns(f_ref.at[frame], r, first, cols)

    def part_step(frame):
        pl.when(frame == 0)(lambda: landed(0))
        for r in range(rows + 2 * HALO):
            spread_columns(x_ref.at[frame], r, jnp.maximum(moved[frame, r].astype(jnp.float32), 0.0), cols)
        none = jnp.zeros_like(coarse[frame, 0])
        first_row(frame, rows - 1)
        part = conv_rows(f_ref.at[frame], rows - 1, 0, 1, cols, w2_ref) + lifted(none, coarse[frame, half - 1])
        part_out[0, frame] = part.astype(jnp.bfloat16)
        first_row(frame, 0)
        part = conv_rows(f_ref.at[frame], -2, 2, 3, cols, w2_ref) + lifted(none, coarse[frame, 0])
        part_out[1, frame] = part.astype(jnp.bfloat16)
        now = frame > 1
        pl.when(has_after & (now | near_after))(lambda: part_up(frame).start())
        pl.when(has_before & (now | near_before))(lambda: part_down(frame).start())

    def held_parts():
        landed(1)
        for frame in range(2):
            pl.when(has_after & near_before)(lambda: part_up(frame).start())
            pl.when(has_before & near_after)(lambda: part_down(frame).start())

    def conv_step(frame):
        for r in range(1, rows - 1):
            first_row(frame, r)
        for r in range(rows):
            near = coarse[frame, r // 2]
            none = jnp.zeros_like(near)
            if r == 0:
                far = jnp.where(has_before, none, near)
            elif r == rows - 1:
                far = jnp.where(has_after, none, near)
            else:
                far = coarse[frame, r // 2 - 1] if r % 2 == 0 else coarse[frame, r // 2 + 1]
            first_tap, last_tap = 1 if r == 0 else 0, 2 if r == rows - 1 else 3
            second = conv_rows(f_ref.at[frame], r - 1, first_tap, last_tap, cols, w2_ref)
            joined = lifted(near, far) + moved[frame, r + HALO].astype(jnp.float32) + second
            if r == 0:
                edges[frame, 0] = joined
            elif r == rows - 1:
                edges[frame, 1] = joined
            else:
                mine[frame, r] = joined.astype(jnp.bfloat16)

    def conv_turn(turn, carry):
        pl.when(turn >= 2)(lambda: conv_step(turn - 2))
        pl.when(turn == 2)(held_parts)
        pl.when(turn < own)(lambda: part_step(turn))
        return carry

    fine_left()
    lax.fori_loop(0, own + 2, conv_turn, 0)

    pl.when(has_after)(lambda: halo_up(pl.ds(*crowd[2]), rest, 0).wait_send())
    pl.when(has_before)(lambda: halo_down(pl.ds(*crowd[2]), rest, 0).wait_send())
    pl.when(has_after)(lambda: ring_up().wait_send())
    pl.when(has_before)(lambda: ring_down().wait_send())
    for shift in range(1, halves):
        ring_pass(shift).wait_send()

    def join_step(frame, carry):
        pl.when(has_before)(lambda: part_up(frame).wait_recv())
        mine[frame, 0] = (edges[frame, 0] + part_in[0, frame].astype(jnp.float32)).astype(jnp.bfloat16)
        pl.when(has_after)(lambda: part_down(frame).wait_recv())
        mine[frame, rows - 1] = (edges[frame, 1] + part_in[1, frame].astype(jnp.float32)).astype(jnp.bfloat16)
        return carry

    lax.fori_loop(0, own, join_step, 0)
    pl.when(has_after)(lambda: to_after(part_out.at[0], part_in.at[0], part_send.at[0], part_recv.at[0, 0]).wait_send())
    pl.when(has_before)(lambda: to_before(part_out.at[1], part_in.at[1], part_send.at[1], part_recv.at[1, 0]).wait_send())


def local(fine, coarse, w_query, w_key, w_value, w_out, conv_first, conv_second):
    own, rows, cols, width = fine.shape
    _, half, small, _ = coarse.shape
    bands, halves = lax.axis_size("space"), lax.axis_size("tm")
    far = own * (halves - 1)
    lots = 4 + CHUNKS
    halved = (2, HEADS, width // HEADS // 2, width)
    any_space = pl.BlockSpec(memory_space=pl.ANY)
    bf16 = jnp.bfloat16
    pos = jnp.asarray(encode(own * halves, width))
    lift = jnp.asarray(lift_matrix(small))
    return pl.pallas_call(
        functools.partial(kernel, bands, halves),
        in_specs=[any_space] * 10,
        out_specs=pl.BlockSpec(memory_space=pltpu.VMEM),
        out_shape=pltpu.VMEM(fine.shape, bf16),
        scratch_shapes=[
            pltpu.VMEM((far, rows, cols, width), bf16),
            pltpu.VMEM((own, rows + 2 * HALO, cols, width), bf16),
            pltpu.VMEM((own, half, small, width), bf16),
            pltpu.VMEM((own, (rows + 2 * HALO) * cols, 3 * width), bf16),
            pltpu.VMEM((own, rows * cols, 3 * width), bf16),
            pltpu.VMEM(pos.shape, jnp.float32),
            pltpu.VMEM((width, width), bf16),
            pltpu.VMEM((width, width), bf16),
            pltpu.VMEM((width, width), bf16),
            pltpu.VMEM(halved, bf16),
            pltpu.VMEM((9 * width, width), bf16),
            pltpu.VMEM((9 * width, width), bf16),
            pltpu.VMEM(lift.shape, bf16),
            pltpu.VMEM((own, 2, cols, width), jnp.float32),
            pltpu.VMEM((2, own, cols, width), bf16),
            pltpu.VMEM((2, own, cols, width), bf16),
            pltpu.VMEM((2, own * halves, cols // STEPS, width), bf16),
            *[pltpu.VMEM((count * 2 * cols // STEPS, width), bf16) for count in (own, own + far, own + far)] * 2,
            pltpu.SemaphoreType.DMA((10,)),
            pltpu.SemaphoreType.DMA((lots,)),
            pltpu.SemaphoreType.DMA((halves - 1,)),
            pltpu.SemaphoreType.DMA((halves - 1, lots)),
            pltpu.SemaphoreType.DMA((2,)),
            pltpu.SemaphoreType.DMA((2, 2)),
            pltpu.SemaphoreType.DMA((2,)),
            pltpu.SemaphoreType.DMA((2, own)),
            pltpu.SemaphoreType.DMA((2,)),
            pltpu.SemaphoreType.DMA((2,)),
            pltpu.SemaphoreType.DMA((halves - 1,)),
            pltpu.SemaphoreType.DMA((halves - 1,)),
        ],
        compiler_params=pltpu.CompilerParams(
            collective_id=0, has_side_effects=True, vmem_limit_bytes=54 * 1024 * 1024
        ),
        name="fused",
    )(
        fine, coarse, pos, w_query, w_key, w_value,
        w_out.reshape(HEADS, 2, width // HEADS // 2, width), conv_first.reshape(9 * width, width), conv_second.reshape(9 * width, width), lift,
    )


def solution(mesh):
    return jax.shard_map(
        local,
        mesh=mesh,
        in_specs=(
            P("tm", "space", None, None),
            P("tm", "space", None, None),
            P(),
            P(),
            P(),
            P(),
            P(),
            P(),
        ),
        out_specs=P("tm", "space", None, None),
        check_vma=False,
    )
```

```python
import functools

import jax
import jax.numpy as jnp
import numpy as np
from jax import lax
from jax.experimental import pallas as pl
from jax.experimental.pallas import tpu as pltpu
from jax.sharding import PartitionSpec as P

HEADS = 8
CHUNKS = 4
STEPS = 8
HALO = 1
LOG2E = 1.4426950408889634
MESH = pl.DeviceIdType.MESH


def encode(frames, width):
    half = width // 2
    inverse = np.exp(-np.log(10000.0) * 2.0 * np.arange(half) / width)
    angles = np.arange(frames)[:, None] * inverse[None, :]
    return np.concatenate([np.sin(angles), np.cos(angles)], axis=1).astype(np.float32)


def lift_matrix(small):
    out = np.arange(2 * small)[:, None]
    source = np.arange(small)[None, :]
    near = out // 2
    far = np.clip(np.where(out % 2 == 0, near - 1, near + 1), 0, small - 1)
    base = 0.75 * (source == near) + 0.25 * (source == far)
    return np.concatenate([0.75 * base, 0.25 * base], axis=1).astype(jnp.bfloat16)


def project(frames, own, pos, wq_ref, wk_ref, wv_ref, query_ref, key_ref, value_ref):
    tile, width = frames[0].shape
    scale = LOG2E / (float(width // HEADS) ** 0.5)
    normed = []
    for x, place in zip(frames, pos):
        hidden = x.astype(jnp.float32) + place
        center = hidden - jnp.mean(hidden, axis=-1, keepdims=True)
        spread = jnp.mean(center * center, axis=-1, keepdims=True)
        normed.append((center * lax.rsqrt(spread + 1e-05)).astype(jnp.bfloat16))
    flat = jnp.concatenate(normed, axis=0)
    query = jnp.dot(flat[: own * tile], wq_ref[...], preferred_element_type=jnp.float32)
    query_ref[...] = (query * scale).astype(jnp.bfloat16)
    key_ref[...] = jnp.dot(flat, wk_ref[...], preferred_element_type=jnp.float32).astype(jnp.bfloat16)
    value_ref[...] = jnp.dot(flat, wv_ref[...], preferred_element_type=jnp.float32).astype(jnp.bfloat16)


def iotas(rows, cols):
    return lax.broadcasted_iota(jnp.int32, (rows, cols), 0), lax.broadcasted_iota(jnp.int32, (rows, cols), 1)


def halve_heads(weight):
    width = weight.shape[1]
    depth = width // HEADS
    half = depth // 2
    source, place = iotas(width, width)
    side, lane = place // (width // 2), lax.rem(place, width // 2)
    wanted = lane // half * depth + side * half + lax.rem(lane, half)
    order = jnp.where(source == wanted, 1.0, 0.0).astype(jnp.bfloat16)
    return jnp.dot(weight, order, preferred_element_type=jnp.float32).astype(jnp.bfloat16)


def mix(tile, query_ref, key_ref, value_ref, wo_ref):
    size, width = query_ref.shape
    own, half = size // tile, width // 2
    query = query_ref[...].reshape(own, tile, width)
    source, place = iotas(2 * width, width)
    same_frame = source // width == place // half
    same_head = lax.rem(source, width) // (width // HEADS) == lax.rem(place, half) // (half // HEADS)
    blocks = jnp.where(same_frame & same_head, 1.0, 0.0).astype(jnp.bfloat16)
    places = [slice(at * tile, (at + 1) * tile) for at in range(key_ref.shape[0] // tile)]
    products = [(query * key_ref[at][None]).reshape(size, width) for at in places]
    scores = []
    for at in range(0, len(places), 2):
        pair = jnp.concatenate(products[at : at + 2], axis=1)
        pair = jnp.dot(pair, blocks, preferred_element_type=jnp.float32)
        scores += [pair[:, :half], pair[:, half:]]
    largest = functools.reduce(jnp.maximum, scores)
    total, summed = None, [None, None]
    for at, score in zip(places, scores):
        power = jnp.exp2(score - largest).reshape(own, tile, half)
        total = power if total is None else total + power
        for side in range(2):
            term = power * value_ref[at, side * half : (side + 1) * half].astype(jnp.float32)[None]
            summed[side] = term if summed[side] is None else summed[side] + term
    inverse = 1.0 / total
    attended = jnp.concatenate([(part * inverse).astype(jnp.bfloat16).reshape(size, half) for part in summed], axis=1)
    branch = jnp.dot(attended, wo_ref[...].reshape(width, width), preferred_element_type=jnp.float32)
    return branch.reshape(own, tile, width)


def spread_columns(ref, at, row, cols):
    column = lax.broadcasted_iota(jnp.int32, row.shape, 0)
    left = jnp.where(column == 0, 0.0, pltpu.roll(row, 1, 0))
    right = jnp.where(column == cols - 1, 0.0, pltpu.roll(row, cols - 1, 0))
    width = row.shape[1]
    ref[at * cols : (at + 1) * cols, :width] = left.astype(jnp.bfloat16)
    ref[at * cols : (at + 1) * cols, width : 2 * width] = row.astype(jnp.bfloat16)
    ref[at * cols : (at + 1) * cols, 2 * width :] = right.astype(jnp.bfloat16)


def conv_rows(ref, start, first, last, cols, weight_ref):
    pieces = [ref[(start + step) * cols : (start + step + 1) * cols, :] for step in range(first, last)]
    depth = ref.shape[1]
    return jnp.dot(
        jnp.concatenate(pieces, axis=1), weight_ref[first * depth : last * depth, :], preferred_element_type=jnp.float32
    )


def kernel(
    bands, halves, fine_ref, coarse_ref, pos_hbm, wq_hbm, wk_hbm, wv_hbm, wo_hbm, w1_hbm, w2_hbm, lift_hbm, mine,
    other, moved, coarse, x_ref, f_ref, pos_ref, wq_ref, wk_ref, wv_ref, wo_ref, w1_ref, w2_ref, lift_ref,
    edges, part_out, part_in, ring, query0, key0, value0, query1, key1, value1,
    weight_sems, local_sems, fine_send, fine_recv, halo_send, halo_recv, part_send, part_recv,
    ring_send, ring_recv, pass_send, pass_recv,
):
    own, rows, cols, width = mine.shape
    half = rows // 2
    span = cols // CHUNKS
    thin = cols // STEPS
    early = own // 2
    pieces = 2 * STEPS - 2
    groups = [(0, thin), (thin, thin), (2 * thin, 2 * thin), (4 * thin, cols - 4 * thin)]
    slabs = [(row, 1, at, size) for at, size in groups for row in (0, rows - 1)]
    slabs += [(1, rows - 2, chunk * span, span) for chunk in range(CHUNKS)]
    lots = [slab // 2 if slab < 2 * len(groups) else slab - len(groups) for slab in range(len(slabs))]
    slots = ((query0, key0, value0), (query1, key1, value1))
    place, core = lax.axis_index("space"), lax.axis_index("tm")
    has_before, has_after = place > 0, place < bands - 1
    near_after = lax.rem(place, 2) == 0
    near_before = jnp.logical_not(near_after)

    def mine_copy(slab):
        row, count, at, size = slabs[slab]
        where = (slice(None), pl.ds(row, count), pl.ds(at, size))
        return pltpu.make_async_copy(fine_ref.at[where], mine.at[where], local_sems.at[lots[slab]])

    def fine_copy(shift, slab):
        row, count, at, size = slabs[slab]
        source = mine if count == 1 else fine_ref
        return pltpu.make_async_remote_copy(
            src_ref=source.at[:, pl.ds(row, count), pl.ds(at, size)],
            dst_ref=other.at[pl.ds((shift - 1) * own, own), pl.ds(row, count), pl.ds(at, size)],
            send_sem=fine_send.at[shift - 1],
            recv_sem=fine_recv.at[shift - 1, lots[slab]],
            device_id={"tm": lax.rem(core + halves - shift, halves)},
            device_id_type=MESH,
        )

    def lot_part(lot):
        if lot < len(groups):
            return (slice(None), pl.ds(0, 2), pl.ds(*groups[lot]))
        row, count, at, size = slabs[lot + len(groups)]
        return (slice(None), pl.ds(row, count), pl.ds(at, size))

    def mine_landed(lot):
        where = lot_part(lot)
        pltpu.make_async_copy(fine_ref.at[where], mine.at[where], local_sems.at[lot]).wait()

    def fine_landed(lot):
        where = lot_part(lot)
        for shift in range(1, halves):
            pltpu.make_async_remote_copy(
                src_ref=mine.at[where],
                dst_ref=other.at[pl.ds((shift - 1) * own, own), *where[1:]],
                send_sem=fine_send.at[shift - 1],
                recv_sem=fine_recv.at[shift - 1, lot],
                device_id={"tm": lax.rem(core + halves - shift, halves)},
                device_id_type=MESH,
            ).wait_recv()

    def fine_left():
        for shift in range(1, halves):
            pltpu.make_async_remote_copy(
                src_ref=mine,
                dst_ref=other.at[pl.ds((shift - 1) * own, own)],
                send_sem=fine_send.at[shift - 1],
                recv_sem=fine_recv.at[shift - 1, 0],
                device_id={"tm": lax.rem(core + halves - shift, halves)},
                device_id_type=MESH,
            ).wait_send()

    def to_after(src, dst, send, recv):
        return pltpu.make_async_remote_copy(
            src_ref=src, dst_ref=dst, send_sem=send, recv_sem=recv, device_id={"space": place + 1}, device_id_type=MESH
        )

    def to_before(src, dst, send, recv):
        return pltpu.make_async_remote_copy(
            src_ref=src, dst_ref=dst, send_sem=send, recv_sem=recv, device_id={"space": place - 1}, device_id_type=MESH
        )

    def part_up(frame):
        return to_after(part_out.at[0, frame], part_in.at[0, frame], part_send.at[0], part_recv.at[0, frame])

    def part_down(frame):
        return to_before(part_out.at[1, frame], part_in.at[1, frame], part_send.at[1], part_recv.at[1, frame])

    def ring_up():
        return to_after(mine.at[:, rows - 1, 0:thin], ring.at[0, 0:own], ring_send.at[0], ring_recv.at[0])

    def ring_down():
        return to_before(mine.at[:, 0, 0:thin], ring.at[1, 0:own], ring_send.at[1], ring_recv.at[1])

    def ring_pass(shift):
        return pltpu.make_async_remote_copy(
            src_ref=ring.at[:, 0:own],
            dst_ref=ring.at[:, pl.ds(shift * own, own)],
            send_sem=pass_send.at[shift - 1],
            recv_sem=pass_recv.at[shift - 1],
            device_id={"tm": lax.rem(core + halves - shift, halves)},
            device_id_type=MESH,
        )

    def halo_up(frames, span_at, late):
        return to_after(
            moved.at[frames, rows : rows + HALO, span_at], moved.at[frames, 0:HALO, span_at],
            halo_send.at[0], halo_recv.at[0, late],
        )

    def halo_down(frames, span_at, late):
        return to_before(
            moved.at[frames, HALO : 2 * HALO, span_at], moved.at[frames, rows + HALO : rows + 2 * HALO, span_at],
            halo_send.at[1], halo_recv.at[1, late],
        )

    crowd = ((0, early), (early, own - early), (0, own))

    def landed(late):
        frames = pl.ds(*crowd[late])
        pl.when(has_before)(lambda: halo_up(frames, rest, late).wait_recv())
        pl.when(has_after)(lambda: halo_down(frames, rest, late).wait_recv())

    rest = pl.ds(thin, cols - thin)
    barrier = pltpu.get_barrier_semaphore()
    for shift in range(1, halves):
        pl.semaphore_signal(barrier, inc=1, device_id={"tm": lax.rem(core + shift, halves)}, device_id_type=MESH)

    @pl.when(has_before)
    def _():
        pl.semaphore_signal(barrier, inc=1, device_id={"space": place - 1}, device_id_type=MESH)

    @pl.when(has_after)
    def _():
        pl.semaphore_signal(barrier, inc=1, device_id={"space": place + 1}, device_id_type=MESH)

    motion_weights = [
        pltpu.make_async_copy(src, dst, weight_sems.at[at])
        for at, (src, dst) in enumerate(
            [(wv_hbm, wv_ref), (pos_hbm, pos_ref), (wq_hbm, wq_ref), (wk_hbm, wk_ref)]
            + [(wo_hbm.at[:, side], wo_ref.at[side]) for side in range(2)]
        )
    ]
    later_weights = [
        pltpu.make_async_copy(src, dst, weight_sems.at[6 + at])
        for at, (src, dst) in enumerate(
            [(lift_hbm, lift_ref), (w1_hbm, w1_ref), (w2_hbm, w2_ref), (coarse_ref, coarse)]
        )
    ]
    for slab in range(4):
        mine_copy(slab).start()
    for copy in motion_weights:
        copy.start()
    for slab in range(4, len(slabs)):
        mine_copy(slab).start()
    for copy in later_weights:
        copy.start()

    @pl.when(jnp.logical_not(has_before))
    def _():
        moved[:, 0:HALO] = jnp.zeros((own, HALO, cols, width), jnp.bfloat16)
        part_in[0] = jnp.zeros((own, cols, width), jnp.bfloat16)
        ring[0, 0:own] = jnp.zeros((own, thin, width), jnp.bfloat16)

    @pl.when(jnp.logical_not(has_after))
    def _():
        moved[:, rows + HALO :] = jnp.zeros((own, HALO, cols, width), jnp.bfloat16)
        part_in[1] = jnp.zeros((own, cols, width), jnp.bfloat16)
        ring[1, 0:own] = jnp.zeros((own, thin, width), jnp.bfloat16)

    peers = halves - 1 + has_before.astype(jnp.int32) + has_after.astype(jnp.int32)
    pl.semaphore_wait(barrier, peers)

    mine_landed(0)
    pl.when(has_after)(lambda: ring_up().start())
    pl.when(has_before)(lambda: ring_down().start())
    for slab in (2, 3, 4, 5, 6, 7, 0, 1, *range(8, len(slabs))):
        if slab in (2, 4, 6):
            mine_landed(lots[slab])
        for shift in range(1, halves):
            fine_copy(shift, slab).start()
    motion_weights[0].wait()
    wv_ref[...] = halve_heads(wv_ref[...])
    for copy in motion_weights[1:]:
        copy.wait()

    pos = []
    for shift in range(halves):
        for frame in range(own):
            pos.append(pos_ref[pl.ds(lax.rem(core + shift, halves) * own + frame, 1), :])

    needs = {0: 1, 1: 2, 3: 3, STEPS - 1: 0}
    for chunk in range(CHUNKS):
        needs[STEPS + max(chunk * STEPS // CHUNKS - 1, 0)] = len(groups) + chunk

    def places_of(tile):
        pair, step = tile // STEPS, lax.rem(tile + 1, STEPS)
        at = pl.ds(pl.multiple_of(step * thin, thin), thin)
        return (pair, at), (rows - 1 - pair, at)

    def arrive(tile):
        for when, lot in needs.items():

            @pl.when(tile == when)
            def _():
                if lot >= len(groups):
                    mine_landed(lot)
                fine_landed(lot)

        pl.when(tile == STEPS - 2)(pass_ring)

    def pass_ring():
        pl.when(has_before)(lambda: ring_up().wait_recv())
        pl.when(has_after)(lambda: ring_down().wait_recv())
        for shift in range(1, halves):
            ring_pass(shift).start()

    def enter_ring(slot):
        frames = [jnp.concatenate([ring[0, frame], ring[1, frame]]) for frame in range(own * halves)]
        project(frames, own, pos, wq_ref, wk_ref, wv_ref, *slots[slot])

    def leave_ring(slot):
        branch = mix(2 * thin, *slots[slot], wo_ref)
        for frame in range(own):
            for side, real in enumerate((has_before, has_after)):
                result = ring[side, frame].astype(jnp.float32) + branch[frame, side * thin : (side + 1) * thin]
                moved[frame, side * (rows + HALO), 0:thin, :] = jnp.where(real, result, 0.0).astype(jnp.bfloat16)

    def enter(tile, slot):
        places = places_of(tile)
        frames = [jnp.concatenate([mine[frame, row, at, :] for row, at in places]) for frame in range(own)]
        frames += [
            jnp.concatenate([other[frame, row, at, :] for row, at in places]) for frame in range(own * (halves - 1))
        ]
        project(frames, own, pos, wq_ref, wk_ref, wv_ref, *slots[slot])

    def leave(tile, slot):
        places = places_of(tile)
        branch = mix(2 * thin, *slots[slot], wo_ref)
        for frame in range(own):
            for n, (row, at) in enumerate(places):
                result = mine[frame, row, at, :].astype(jnp.float32) + branch[frame, n * thin : (n + 1) * thin]
                moved[frame, row + HALO, at, :] = result.astype(jnp.bfloat16)

    def hand_over(tile):
        now = tile < STEPS - 1
        columns = pl.ds(pl.multiple_of((tile + 1) * thin, thin), thin)
        pl.when(has_after & now)(lambda: halo_up(pl.ds(*crowd[0]), columns, 0).start())
        pl.when(has_before & now)(lambda: halo_down(pl.ds(*crowd[0]), columns, 0).start())
        local, transit = tile == STEPS - 1, tile == 12
        up_if = has_after & ((near_after & local) | (near_before & transit))
        down_if = has_before & ((near_before & local) | (near_after & transit))
        pl.when(up_if)(lambda: halo_up(pl.ds(*crowd[1]), rest, 1).start())
        pl.when(down_if)(lambda: halo_down(pl.ds(*crowd[1]), rest, 1).start())

    def turn(tile, slot):
        arrive(tile + 1)
        leave(tile, slot)
        enter(tile + 1, 1 - slot)
        hand_over(tile)

    def two_turns(step, carry):
        turn(2 * step, 0)
        turn(2 * step + 1, 1)
        return carry

    tiles = STEPS * (rows // 2)
    arrive(0)
    enter(0, 0)
    lax.fori_loop(0, tiles // 2 - 1, two_turns, 0)
    turn(tiles - 2, 0)
    for shift in range(1, halves):
        ring_pass(shift).wait_recv()
    leave(tiles - 1, 1)
    enter_ring(0)
    leave_ring(0)

    for copy in later_weights:
        copy.wait()

    def lifted(near, far):
        return jnp.dot(lift_ref[...], jnp.concatenate([near, far], axis=0), preferred_element_type=jnp.float32)

    def first_row(frame, r):
        first = conv_rows(x_ref.at[frame], r, 0, 3, cols, w1_ref)
        first = jnp.maximum(first, 0.0).astype(jnp.bfloat16).astype(jnp.float32)
        spread_columns(f_ref.at[frame], r, first, cols)

    def part_step(frame):
        pl.when(frame == 0)(lambda: landed(0))
        for r in range(rows + 2 * HALO):
            spread_columns(x_ref.at[frame], r, jnp.maximum(moved[frame, r].astype(jnp.float32), 0.0), cols)
        none = jnp.zeros_like(coarse[frame, 0])
        first_row(frame, rows - 1)
        part = conv_rows(f_ref.at[frame], rows - 1, 0, 1, cols, w2_ref) + lifted(none, coarse[frame, half - 1])
        part_out[0, frame] = part.astype(jnp.bfloat16)
        first_row(frame, 0)
        part = conv_rows(f_ref.at[frame], -2, 2, 3, cols, w2_ref) + lifted(none, coarse[frame, 0])
        part_out[1, frame] = part.astype(jnp.bfloat16)
        pl.when(has_after & near_after)(lambda: part_up(frame).start())
        pl.when(has_before & near_before)(lambda: part_down(frame).start())

    def far_part(frame):
        pl.when(has_after & near_before)(lambda: part_up(frame).start())
        pl.when(has_before & near_after)(lambda: part_down(frame).start())

    def held_parts():
        landed(1)
        for frame in range(2):
            pl.when(has_after & near_before)(lambda: part_up(frame).start())
            pl.when(has_before & near_after)(lambda: part_down(frame).start())

    def conv_step(frame):
        for r in range(1, rows - 1):
            first_row(frame, r)
        for r in range(rows):
            near = coarse[frame, r // 2]
            none = jnp.zeros_like(near)
            if r == 0:
                far = jnp.where(has_before, none, near)
            elif r == rows - 1:
                far = jnp.where(has_after, none, near)
            else:
                far = coarse[frame, r // 2 - 1] if r % 2 == 0 else coarse[frame, r // 2 + 1]
            first_tap, last_tap = 1 if r == 0 else 0, 2 if r == rows - 1 else 3
            second = conv_rows(f_ref.at[frame], r - 1, first_tap, last_tap, cols, w2_ref)
            joined = lifted(near, far) + moved[frame, r + HALO].astype(jnp.float32) + second
            if r == 0:
                edges[frame, 0] = joined
            elif r == rows - 1:
                edges[frame, 1] = joined
            else:
                mine[frame, r] = joined.astype(jnp.bfloat16)

    def conv_turn(turn, carry):
        pl.when(turn >= 2)(lambda: conv_step(turn - 2))
        pl.when(turn == 2)(held_parts)
        pl.when(turn < own)(lambda: part_step(turn))
        pl.when(turn > 3)(lambda: far_part(turn - 2))
        return carry

    fine_left()
    lax.fori_loop(0, own + 2, conv_turn, 0)

    pl.when(has_after)(lambda: halo_up(pl.ds(*crowd[2]), rest, 0).wait_send())
    pl.when(has_before)(lambda: halo_down(pl.ds(*crowd[2]), rest, 0).wait_send())
    pl.when(has_after)(lambda: ring_up().wait_send())
    pl.when(has_before)(lambda: ring_down().wait_send())
    for shift in range(1, halves):
        ring_pass(shift).wait_send()

    def join_step(frame, carry):
        pl.when(has_before)(lambda: part_up(frame).wait_recv())
        mine[frame, 0] = (edges[frame, 0] + part_in[0, frame].astype(jnp.float32)).astype(jnp.bfloat16)
        pl.when(has_after)(lambda: part_down(frame).wait_recv())
        mine[frame, rows - 1] = (edges[frame, 1] + part_in[1, frame].astype(jnp.float32)).astype(jnp.bfloat16)
        return carry

    lax.fori_loop(0, own, join_step, 0)
    pl.when(has_after)(lambda: to_after(part_out.at[0], part_in.at[0], part_send.at[0], part_recv.at[0, 0]).wait_send())
    pl.when(has_before)(lambda: to_before(part_out.at[1], part_in.at[1], part_send.at[1], part_recv.at[1, 0]).wait_send())


def local(fine, coarse, w_query, w_key, w_value, w_out, conv_first, conv_second):
    own, rows, cols, width = fine.shape
    _, half, small, _ = coarse.shape
    bands, halves = lax.axis_size("space"), lax.axis_size("tm")
    far = own * (halves - 1)
    lots = 4 + CHUNKS
    halved = (2, HEADS, width // HEADS // 2, width)
    any_space = pl.BlockSpec(memory_space=pl.ANY)
    bf16 = jnp.bfloat16
    pos = jnp.asarray(encode(own * halves, width))
    lift = jnp.asarray(lift_matrix(small))
    return pl.pallas_call(
        functools.partial(kernel, bands, halves),
        in_specs=[any_space] * 10,
        out_specs=pl.BlockSpec(memory_space=pltpu.VMEM),
        out_shape=pltpu.VMEM(fine.shape, bf16),
        scratch_shapes=[
            pltpu.VMEM((far, rows, cols, width), bf16),
            pltpu.VMEM((own, rows + 2 * HALO, cols, width), bf16),
            pltpu.VMEM((own, half, small, width), bf16),
            pltpu.VMEM((own, (rows + 2 * HALO) * cols, 3 * width), bf16),
            pltpu.VMEM((own, rows * cols, 3 * width), bf16),
            pltpu.VMEM(pos.shape, jnp.float32),
            pltpu.VMEM((width, width), bf16),
            pltpu.VMEM((width, width), bf16),
            pltpu.VMEM((width, width), bf16),
            pltpu.VMEM(halved, bf16),
            pltpu.VMEM((9 * width, width), bf16),
            pltpu.VMEM((9 * width, width), bf16),
            pltpu.VMEM(lift.shape, bf16),
            pltpu.VMEM((own, 2, cols, width), jnp.float32),
            pltpu.VMEM((2, own, cols, width), bf16),
            pltpu.VMEM((2, own, cols, width), bf16),
            pltpu.VMEM((2, own * halves, cols // STEPS, width), bf16),
            *[pltpu.VMEM((count * 2 * cols // STEPS, width), bf16) for count in (own, own + far, own + far)] * 2,
            pltpu.SemaphoreType.DMA((10,)),
            pltpu.SemaphoreType.DMA((lots,)),
            pltpu.SemaphoreType.DMA((halves - 1,)),
            pltpu.SemaphoreType.DMA((halves - 1, lots)),
            pltpu.SemaphoreType.DMA((2,)),
            pltpu.SemaphoreType.DMA((2, 2)),
            pltpu.SemaphoreType.DMA((2,)),
            pltpu.SemaphoreType.DMA((2, own)),
            pltpu.SemaphoreType.DMA((2,)),
            pltpu.SemaphoreType.DMA((2,)),
            pltpu.SemaphoreType.DMA((halves - 1,)),
            pltpu.SemaphoreType.DMA((halves - 1,)),
        ],
        compiler_params=pltpu.CompilerParams(
            collective_id=0, has_side_effects=True, vmem_limit_bytes=54 * 1024 * 1024
        ),
        name="fused",
    )(
        fine, coarse, pos, w_query, w_key, w_value,
        w_out.reshape(HEADS, 2, width // HEADS // 2, width), conv_first.reshape(9 * width, width), conv_second.reshape(9 * width, width), lift,
    )


def solution(mesh):
    return jax.shard_map(
        local,
        mesh=mesh,
        in_specs=(
            P("tm", "space", None, None),
            P("tm", "space", None, None),
            P(),
            P(),
            P(),
            P(),
            P(),
            P(),
        ),
        out_specs=P("tm", "space", None, None),
        check_vma=False,
    )
```

```python
import functools

import jax
import jax.numpy as jnp
import numpy as np
from jax import lax
from jax.experimental import pallas as pl
from jax.experimental.pallas import tpu as pltpu
from jax.sharding import PartitionSpec as P

HEADS = 8
CHUNKS = 2
STEPS = 8
HALO = 1
LOG2E = 1.4426950408889634
MESH = pl.DeviceIdType.MESH


def encode(frames, width):
    half = width // 2
    inverse = np.exp(-np.log(10000.0) * 2.0 * np.arange(half) / width)
    angles = np.arange(frames)[:, None] * inverse[None, :]
    return np.concatenate([np.sin(angles), np.cos(angles)], axis=1).astype(np.float32)


def lift_matrix(small):
    out = np.arange(2 * small)[:, None]
    source = np.arange(small)[None, :]
    near = out // 2
    far = np.clip(np.where(out % 2 == 0, near - 1, near + 1), 0, small - 1)
    base = 0.75 * (source == near) + 0.25 * (source == far)
    return np.concatenate([0.75 * base, 0.25 * base], axis=1).astype(jnp.bfloat16)


def project(frames, own, pos, wq_ref, wk_ref, wv_ref, query_ref, key_ref, value_ref):
    tile, width = frames[0].shape
    scale = LOG2E / (float(width // HEADS) ** 0.5)
    normed = []
    for x, place in zip(frames, pos):
        hidden = x.astype(jnp.float32) + place
        center = hidden - jnp.mean(hidden, axis=-1, keepdims=True)
        spread = jnp.mean(center * center, axis=-1, keepdims=True)
        normed.append((center * lax.rsqrt(spread + 1e-05)).astype(jnp.bfloat16))
    flat = jnp.concatenate(normed, axis=0)
    query = jnp.dot(flat[: own * tile], wq_ref[...], preferred_element_type=jnp.float32)
    query_ref[...] = (query * scale).astype(jnp.bfloat16)
    key_ref[...] = jnp.dot(flat, wk_ref[...], preferred_element_type=jnp.float32).astype(jnp.bfloat16)
    value_ref[...] = jnp.dot(flat, wv_ref[...], preferred_element_type=jnp.float32).astype(jnp.bfloat16)


def iotas(rows, cols):
    return lax.broadcasted_iota(jnp.int32, (rows, cols), 0), lax.broadcasted_iota(jnp.int32, (rows, cols), 1)


def halve_heads(weight):
    width = weight.shape[1]
    depth = width // HEADS
    half = depth // 2
    source, place = iotas(width, width)
    side, lane = place // (width // 2), lax.rem(place, width // 2)
    wanted = lane // half * depth + side * half + lax.rem(lane, half)
    order = jnp.where(source == wanted, 1.0, 0.0).astype(jnp.bfloat16)
    return jnp.dot(weight, order, preferred_element_type=jnp.float32).astype(jnp.bfloat16)


def mix(tile, query_ref, key_ref, value_ref, wo_ref):
    size, width = query_ref.shape
    own, half = size // tile, width // 2
    query = query_ref[...].reshape(own, tile, width)
    source, place = iotas(2 * width, width)
    same_frame = source // width == place // half
    same_head = lax.rem(source, width) // (width // HEADS) == lax.rem(place, half) // (half // HEADS)
    blocks = jnp.where(same_frame & same_head, 1.0, 0.0).astype(jnp.bfloat16)
    places = [slice(at * tile, (at + 1) * tile) for at in range(key_ref.shape[0] // tile)]
    products = [(query * key_ref[at][None]).reshape(size, width) for at in places]
    scores = []
    for at in range(0, len(places), 2):
        pair = jnp.concatenate(products[at : at + 2], axis=1)
        pair = jnp.dot(pair, blocks, preferred_element_type=jnp.float32)
        scores += [pair[:, :half], pair[:, half:]]
    largest = functools.reduce(jnp.maximum, scores)
    total, summed = None, [None, None]
    for at, score in zip(places, scores):
        power = jnp.exp2(score - largest).reshape(own, tile, half)
        total = power if total is None else total + power
        for side in range(2):
            term = power * value_ref[at, side * half : (side + 1) * half].astype(jnp.float32)[None]
            summed[side] = term if summed[side] is None else summed[side] + term
    inverse = 1.0 / total
    attended = jnp.concatenate([(part * inverse).astype(jnp.bfloat16).reshape(size, half) for part in summed], axis=1)
    branch = jnp.dot(attended, wo_ref[...].reshape(width, width), preferred_element_type=jnp.float32)
    return branch.reshape(own, tile, width)


def spread_columns(ref, at, row, cols):
    column = lax.broadcasted_iota(jnp.int32, row.shape, 0)
    left = jnp.where(column == 0, 0.0, pltpu.roll(row, 1, 0))
    right = jnp.where(column == cols - 1, 0.0, pltpu.roll(row, cols - 1, 0))
    width = row.shape[1]
    ref[at * cols : (at + 1) * cols, :width] = left.astype(jnp.bfloat16)
    ref[at * cols : (at + 1) * cols, width : 2 * width] = row.astype(jnp.bfloat16)
    ref[at * cols : (at + 1) * cols, 2 * width :] = right.astype(jnp.bfloat16)


def conv_rows(ref, start, first, last, cols, weight_ref):
    pieces = [ref[(start + step) * cols : (start + step + 1) * cols, :] for step in range(first, last)]
    depth = ref.shape[1]
    return jnp.dot(
        jnp.concatenate(pieces, axis=1), weight_ref[first * depth : last * depth, :], preferred_element_type=jnp.float32
    )


def kernel(
    bands, halves, fine_ref, coarse_ref, pos_hbm, wq_hbm, wk_hbm, wv_hbm, wo_hbm, w1_hbm, w2_hbm, lift_hbm, mine,
    other, moved, coarse, x_ref, f_ref, pos_ref, wq_ref, wk_ref, wv_ref, wo_ref, w1_ref, w2_ref, lift_ref,
    edges, part_out, part_in, ring, query0, key0, value0, query1, key1, value1,
    weight_sems, local_sems, fine_send, fine_recv, halo_send, halo_recv, part_send, part_recv,
    ring_send, ring_recv, pass_send, pass_recv,
):
    own, rows, cols, width = mine.shape
    half = rows // 2
    span = cols // CHUNKS
    thin = cols // STEPS
    early = own // 2
    pieces = 2 * STEPS - 2
    groups = [(0, thin), (thin, thin), (2 * thin, 2 * thin), (4 * thin, cols - 4 * thin)]
    slabs = [(row, 1, at, size) for at, size in groups for row in (0, rows - 1)]
    slabs += [(1, rows - 2, chunk * span, span) for chunk in range(CHUNKS)]
    lots = [slab // 2 if slab < 2 * len(groups) else slab - len(groups) for slab in range(len(slabs))]
    slots = ((query0, key0, value0), (query1, key1, value1))
    place, core = lax.axis_index("space"), lax.axis_index("tm")
    has_before, has_after = place > 0, place < bands - 1
    near_after = lax.rem(place, 2) == 0
    near_before = jnp.logical_not(near_after)

    def mine_copy(slab):
        row, count, at, size = slabs[slab]
        where = (slice(None), pl.ds(row, count), pl.ds(at, size))
        return pltpu.make_async_copy(fine_ref.at[where], mine.at[where], local_sems.at[lots[slab]])

    def fine_copy(shift, slab):
        row, count, at, size = slabs[slab]
        source = mine if count == 1 else fine_ref
        return pltpu.make_async_remote_copy(
            src_ref=source.at[:, pl.ds(row, count), pl.ds(at, size)],
            dst_ref=other.at[pl.ds((shift - 1) * own, own), pl.ds(row, count), pl.ds(at, size)],
            send_sem=fine_send.at[shift - 1],
            recv_sem=fine_recv.at[shift - 1, lots[slab]],
            device_id={"tm": lax.rem(core + halves - shift, halves)},
            device_id_type=MESH,
        )

    def lot_part(lot):
        if lot < len(groups):
            return (slice(None), pl.ds(0, 2), pl.ds(*groups[lot]))
        row, count, at, size = slabs[lot + len(groups)]
        return (slice(None), pl.ds(row, count), pl.ds(at, size))

    def mine_landed(lot):
        where = lot_part(lot)
        pltpu.make_async_copy(fine_ref.at[where], mine.at[where], local_sems.at[lot]).wait()

    def fine_landed(lot):
        where = lot_part(lot)
        for shift in range(1, halves):
            pltpu.make_async_remote_copy(
                src_ref=mine.at[where],
                dst_ref=other.at[pl.ds((shift - 1) * own, own), *where[1:]],
                send_sem=fine_send.at[shift - 1],
                recv_sem=fine_recv.at[shift - 1, lot],
                device_id={"tm": lax.rem(core + halves - shift, halves)},
                device_id_type=MESH,
            ).wait_recv()

    def fine_left():
        for shift in range(1, halves):
            pltpu.make_async_remote_copy(
                src_ref=mine,
                dst_ref=other.at[pl.ds((shift - 1) * own, own)],
                send_sem=fine_send.at[shift - 1],
                recv_sem=fine_recv.at[shift - 1, 0],
                device_id={"tm": lax.rem(core + halves - shift, halves)},
                device_id_type=MESH,
            ).wait_send()

    def to_after(src, dst, send, recv):
        return pltpu.make_async_remote_copy(
            src_ref=src, dst_ref=dst, send_sem=send, recv_sem=recv, device_id={"space": place + 1}, device_id_type=MESH
        )

    def to_before(src, dst, send, recv):
        return pltpu.make_async_remote_copy(
            src_ref=src, dst_ref=dst, send_sem=send, recv_sem=recv, device_id={"space": place - 1}, device_id_type=MESH
        )

    def part_up(frame):
        return to_after(part_out.at[0, frame], part_in.at[0, frame], part_send.at[0], part_recv.at[0, frame])

    def part_down(frame):
        return to_before(part_out.at[1, frame], part_in.at[1, frame], part_send.at[1], part_recv.at[1, frame])

    def ring_up():
        return to_after(mine.at[:, rows - 1, 0:thin], ring.at[0, 0:own], ring_send.at[0], ring_recv.at[0])

    def ring_down():
        return to_before(mine.at[:, 0, 0:thin], ring.at[1, 0:own], ring_send.at[1], ring_recv.at[1])

    def ring_pass(shift):
        return pltpu.make_async_remote_copy(
            src_ref=ring.at[:, 0:own],
            dst_ref=ring.at[:, pl.ds(shift * own, own)],
            send_sem=pass_send.at[shift - 1],
            recv_sem=pass_recv.at[shift - 1],
            device_id={"tm": lax.rem(core + halves - shift, halves)},
            device_id_type=MESH,
        )

    def halo_up(frames, span_at, late):
        return to_after(
            moved.at[frames, rows : rows + HALO, span_at], moved.at[frames, 0:HALO, span_at],
            halo_send.at[0], halo_recv.at[0, late],
        )

    def halo_down(frames, span_at, late):
        return to_before(
            moved.at[frames, HALO : 2 * HALO, span_at], moved.at[frames, rows + HALO : rows + 2 * HALO, span_at],
            halo_send.at[1], halo_recv.at[1, late],
        )

    crowd = ((0, early), (early, own - early), (0, own))

    def landed(late):
        frames = pl.ds(*crowd[late])
        pl.when(has_before)(lambda: halo_up(frames, rest, late).wait_recv())
        pl.when(has_after)(lambda: halo_down(frames, rest, late).wait_recv())

    rest = pl.ds(thin, cols - thin)
    barrier = pltpu.get_barrier_semaphore()
    for shift in range(1, halves):
        pl.semaphore_signal(barrier, inc=1, device_id={"tm": lax.rem(core + shift, halves)}, device_id_type=MESH)

    @pl.when(has_before)
    def _():
        pl.semaphore_signal(barrier, inc=1, device_id={"space": place - 1}, device_id_type=MESH)

    @pl.when(has_after)
    def _():
        pl.semaphore_signal(barrier, inc=1, device_id={"space": place + 1}, device_id_type=MESH)

    motion_weights = [
        pltpu.make_async_copy(src, dst, weight_sems.at[at])
        for at, (src, dst) in enumerate(
            [(wv_hbm, wv_ref), (pos_hbm, pos_ref), (wq_hbm, wq_ref), (wk_hbm, wk_ref)]
            + [(wo_hbm.at[:, side], wo_ref.at[side]) for side in range(2)]
        )
    ]
    later_weights = [
        pltpu.make_async_copy(src, dst, weight_sems.at[6 + at])
        for at, (src, dst) in enumerate(
            [(lift_hbm, lift_ref), (w1_hbm, w1_ref), (w2_hbm, w2_ref), (coarse_ref, coarse)]
        )
    ]
    for slab in range(4):
        mine_copy(slab).start()
    for copy in motion_weights:
        copy.start()
    for slab in range(4, len(slabs)):
        mine_copy(slab).start()
    for copy in later_weights:
        copy.start()

    @pl.when(jnp.logical_not(has_before))
    def _():
        moved[:, 0:HALO] = jnp.zeros((own, HALO, cols, width), jnp.bfloat16)
        part_in[0] = jnp.zeros((own, cols, width), jnp.bfloat16)
        ring[0, 0:own] = jnp.zeros((own, thin, width), jnp.bfloat16)

    @pl.when(jnp.logical_not(has_after))
    def _():
        moved[:, rows + HALO :] = jnp.zeros((own, HALO, cols, width), jnp.bfloat16)
        part_in[1] = jnp.zeros((own, cols, width), jnp.bfloat16)
        ring[1, 0:own] = jnp.zeros((own, thin, width), jnp.bfloat16)

    motion_weights[0].wait()
    wv_ref[...] = halve_heads(wv_ref[...])
    peers = halves - 1 + has_before.astype(jnp.int32) + has_after.astype(jnp.int32)
    pl.semaphore_wait(barrier, peers)

    mine_landed(0)
    pl.when(has_after)(lambda: ring_up().start())
    pl.when(has_before)(lambda: ring_down().start())
    for slab in (2, 3, 4, 5, 6, 7, 0, 1, *range(8, len(slabs))):
        if slab in (2, 4, 6):
            mine_landed(lots[slab])
        for shift in range(1, halves):
            fine_copy(shift, slab).start()
    for copy in motion_weights[1:]:
        copy.wait()

    pos = []
    for shift in range(halves):
        for frame in range(own):
            pos.append(pos_ref[pl.ds(lax.rem(core + shift, halves) * own + frame, 1), :])

    needs = {0: 1, 1: 2, 3: 3, STEPS - 1: 0}
    for chunk in range(CHUNKS):
        needs[STEPS + max(chunk * STEPS // CHUNKS - 1, 0)] = len(groups) + chunk

    def places_of(tile):
        pair, step = tile // STEPS, lax.rem(tile + 1, STEPS)
        at = pl.ds(pl.multiple_of(step * thin, thin), thin)
        return (pair, at), (rows - 1 - pair, at)

    def arrive(tile):
        for when, lot in needs.items():

            @pl.when(tile == when)
            def _():
                if lot >= len(groups):
                    mine_landed(lot)
                fine_landed(lot)

        pl.when(tile == STEPS - 2)(pass_ring)

    def pass_ring():
        pl.when(has_before)(lambda: ring_up().wait_recv())
        pl.when(has_after)(lambda: ring_down().wait_recv())
        for shift in range(1, halves):
            ring_pass(shift).start()

    def enter_ring(slot):
        frames = [jnp.concatenate([ring[0, frame], ring[1, frame]]) for frame in range(own * halves)]
        project(frames, own, pos, wq_ref, wk_ref, wv_ref, *slots[slot])

    def leave_ring(slot):
        branch = mix(2 * thin, *slots[slot], wo_ref)
        for frame in range(own):
            for side, real in enumerate((has_before, has_after)):
                result = ring[side, frame].astype(jnp.float32) + branch[frame, side * thin : (side + 1) * thin]
                moved[frame, side * (rows + HALO), 0:thin, :] = jnp.where(real, result, 0.0).astype(jnp.bfloat16)

    def enter(tile, slot):
        places = places_of(tile)
        frames = [jnp.concatenate([mine[frame, row, at, :] for row, at in places]) for frame in range(own)]
        frames += [
            jnp.concatenate([other[frame, row, at, :] for row, at in places]) for frame in range(own * (halves - 1))
        ]
        project(frames, own, pos, wq_ref, wk_ref, wv_ref, *slots[slot])

    def leave(tile, slot):
        places = places_of(tile)
        branch = mix(2 * thin, *slots[slot], wo_ref)
        for frame in range(own):
            for n, (row, at) in enumerate(places):
                result = mine[frame, row, at, :].astype(jnp.float32) + branch[frame, n * thin : (n + 1) * thin]
                moved[frame, row + HALO, at, :] = result.astype(jnp.bfloat16)

    def hand_over(tile):
        now = tile < STEPS - 1
        columns = pl.ds(pl.multiple_of((tile + 1) * thin, thin), thin)
        pl.when(has_after & now)(lambda: halo_up(pl.ds(*crowd[0]), columns, 0).start())
        pl.when(has_before & now)(lambda: halo_down(pl.ds(*crowd[0]), columns, 0).start())
        local, transit = tile == STEPS - 1, tile == 12
        up_if = has_after & ((near_after & local) | (near_before & transit))
        down_if = has_before & ((near_before & local) | (near_after & transit))
        pl.when(up_if)(lambda: halo_up(pl.ds(*crowd[1]), rest, 1).start())
        pl.when(down_if)(lambda: halo_down(pl.ds(*crowd[1]), rest, 1).start())

    def turn(tile, slot):
        arrive(tile + 1)
        leave(tile, slot)
        enter(tile + 1, 1 - slot)
        hand_over(tile)

    def two_turns(step, carry):
        turn(2 * step, 0)
        turn(2 * step + 1, 1)
        return carry

    tiles = STEPS * (rows // 2)
    arrive(0)
    enter(0, 0)
    lax.fori_loop(0, tiles // 2 - 1, two_turns, 0)
    turn(tiles - 2, 0)
    for shift in range(1, halves):
        ring_pass(shift).wait_recv()
    leave(tiles - 1, 1)
    enter_ring(0)
    leave_ring(0)

    for copy in later_weights:
        copy.wait()

    def lifted(near, far):
        return jnp.dot(lift_ref[...], jnp.concatenate([near, far], axis=0), preferred_element_type=jnp.float32)

    def first_row(frame, r):
        first = conv_rows(x_ref.at[frame], r, 0, 3, cols, w1_ref)
        first = jnp.maximum(first, 0.0).astype(jnp.bfloat16).astype(jnp.float32)
        spread_columns(f_ref.at[frame], r, first, cols)

    def part_step(frame):
        pl.when(frame == 0)(lambda: landed(0))
        for r in range(rows + 2 * HALO):
            spread_columns(x_ref.at[frame], r, jnp.maximum(moved[frame, r].astype(jnp.float32), 0.0), cols)
        none = jnp.zeros_like(coarse[frame, 0])
        first_row(frame, rows - 1)
        part = conv_rows(f_ref.at[frame], rows - 1, 0, 1, cols, w2_ref) + lifted(none, coarse[frame, half - 1])
        part_out[0, frame] = part.astype(jnp.bfloat16)
        first_row(frame, 0)
        part = conv_rows(f_ref.at[frame], -2, 2, 3, cols, w2_ref) + lifted(none, coarse[frame, 0])
        part_out[1, frame] = part.astype(jnp.bfloat16)
        pl.when(has_after & near_after)(lambda: part_up(frame).start())
        pl.when(has_before & near_before)(lambda: part_down(frame).start())

    def far_part(frame):
        pl.when(has_after & near_before)(lambda: part_up(frame).start())
        pl.when(has_before & near_after)(lambda: part_down(frame).start())

    def held_parts():
        landed(1)
        for frame in range(2):
            pl.when(has_after & near_before)(lambda: part_up(frame).start())
            pl.when(has_before & near_after)(lambda: part_down(frame).start())

    def conv_step(frame):
        for r in range(1, rows - 1):
            first_row(frame, r)
        for r in range(rows):
            near = coarse[frame, r // 2]
            none = jnp.zeros_like(near)
            if r == 0:
                far = jnp.where(has_before, none, near)
            elif r == rows - 1:
                far = jnp.where(has_after, none, near)
            else:
                far = coarse[frame, r // 2 - 1] if r % 2 == 0 else coarse[frame, r // 2 + 1]
            first_tap, last_tap = 1 if r == 0 else 0, 2 if r == rows - 1 else 3
            second = conv_rows(f_ref.at[frame], r - 1, first_tap, last_tap, cols, w2_ref)
            joined = lifted(near, far) + moved[frame, r + HALO].astype(jnp.float32) + second
            if r == 0:
                edges[frame, 0] = joined
            elif r == rows - 1:
                edges[frame, 1] = joined
            else:
                mine[frame, r] = joined.astype(jnp.bfloat16)

    def conv_turn(turn, carry):
        pl.when(turn >= 2)(lambda: conv_step(turn - 2))
        pl.when(turn == 2)(held_parts)
        pl.when(turn < own)(lambda: part_step(turn))
        pl.when(turn > 3)(lambda: far_part(turn - 2))
        return carry

    fine_left()
    lax.fori_loop(0, own + 2, conv_turn, 0)

    pl.when(has_after)(lambda: halo_up(pl.ds(*crowd[2]), rest, 0).wait_send())
    pl.when(has_before)(lambda: halo_down(pl.ds(*crowd[2]), rest, 0).wait_send())
    pl.when(has_after)(lambda: ring_up().wait_send())
    pl.when(has_before)(lambda: ring_down().wait_send())
    for shift in range(1, halves):
        ring_pass(shift).wait_send()

    def join_step(frame, carry):
        pl.when(has_before)(lambda: part_up(frame).wait_recv())
        mine[frame, 0] = (edges[frame, 0] + part_in[0, frame].astype(jnp.float32)).astype(jnp.bfloat16)
        pl.when(has_after)(lambda: part_down(frame).wait_recv())
        mine[frame, rows - 1] = (edges[frame, 1] + part_in[1, frame].astype(jnp.float32)).astype(jnp.bfloat16)
        return carry

    lax.fori_loop(0, own, join_step, 0)
    pl.when(has_after)(lambda: to_after(part_out.at[0], part_in.at[0], part_send.at[0], part_recv.at[0, 0]).wait_send())
    pl.when(has_before)(lambda: to_before(part_out.at[1], part_in.at[1], part_send.at[1], part_recv.at[1, 0]).wait_send())


def local(fine, coarse, w_query, w_key, w_value, w_out, conv_first, conv_second):
    own, rows, cols, width = fine.shape
    _, half, small, _ = coarse.shape
    bands, halves = lax.axis_size("space"), lax.axis_size("tm")
    far = own * (halves - 1)
    lots = 4 + CHUNKS
    halved = (2, HEADS, width // HEADS // 2, width)
    any_space = pl.BlockSpec(memory_space=pl.ANY)
    bf16 = jnp.bfloat16
    pos = jnp.asarray(encode(own * halves, width))
    lift = jnp.asarray(lift_matrix(small))
    return pl.pallas_call(
        functools.partial(kernel, bands, halves),
        in_specs=[any_space] * 10,
        out_specs=pl.BlockSpec(memory_space=pltpu.VMEM),
        out_shape=pltpu.VMEM(fine.shape, bf16),
        scratch_shapes=[
            pltpu.VMEM((far, rows, cols, width), bf16),
            pltpu.VMEM((own, rows + 2 * HALO, cols, width), bf16),
            pltpu.VMEM((own, half, small, width), bf16),
            pltpu.VMEM((own, (rows + 2 * HALO) * cols, 3 * width), bf16),
            pltpu.VMEM((own, rows * cols, 3 * width), bf16),
            pltpu.VMEM(pos.shape, jnp.float32),
            pltpu.VMEM((width, width), bf16),
            pltpu.VMEM((width, width), bf16),
            pltpu.VMEM((width, width), bf16),
            pltpu.VMEM(halved, bf16),
            pltpu.VMEM((9 * width, width), bf16),
            pltpu.VMEM((9 * width, width), bf16),
            pltpu.VMEM(lift.shape, bf16),
            pltpu.VMEM((own, 2, cols, width), jnp.float32),
            pltpu.VMEM((2, own, cols, width), bf16),
            pltpu.VMEM((2, own, cols, width), bf16),
            pltpu.VMEM((2, own * halves, cols // STEPS, width), bf16),
            *[pltpu.VMEM((count * 2 * cols // STEPS, width), bf16) for count in (own, own + far, own + far)] * 2,
            pltpu.SemaphoreType.DMA((10,)),
            pltpu.SemaphoreType.DMA((lots,)),
            pltpu.SemaphoreType.DMA((halves - 1,)),
            pltpu.SemaphoreType.DMA((halves - 1, lots)),
            pltpu.SemaphoreType.DMA((2,)),
            pltpu.SemaphoreType.DMA((2, 2)),
            pltpu.SemaphoreType.DMA((2,)),
            pltpu.SemaphoreType.DMA((2, own)),
            pltpu.SemaphoreType.DMA((2,)),
            pltpu.SemaphoreType.DMA((2,)),
            pltpu.SemaphoreType.DMA((halves - 1,)),
            pltpu.SemaphoreType.DMA((halves - 1,)),
        ],
        compiler_params=pltpu.CompilerParams(
            collective_id=0, has_side_effects=True, vmem_limit_bytes=54 * 1024 * 1024
        ),
        name="fused",
    )(
        fine, coarse, pos, w_query, w_key, w_value,
        w_out.reshape(HEADS, 2, width // HEADS // 2, width), conv_first.reshape(9 * width, width), conv_second.reshape(9 * width, width), lift,
    )


def solution(mesh):
    return jax.shard_map(
        local,
        mesh=mesh,
        in_specs=(
            P("tm", "space", None, None),
            P("tm", "space", None, None),
            P(),
            P(),
            P(),
            P(),
            P(),
            P(),
        ),
        out_specs=P("tm", "space", None, None),
        check_vma=False,
    )
```
